256 devices in a mesh: blk: 32 (over x, y, z_lo), uly: 8 (over z_hi, core).
Axes of the slice: x: 4, y: 4, z: 8 (z_hi: 4, z_lo: 2; z = z_hi * 2 + z_lo), core: 2. Of those that a mesh axis runs over, the one named last changes fastest.
Arguments:
- self_query: bfloat16 [10240, 5120], P(('blk', 'uly')), may hold values from -8 to 8
- self_key: bfloat16 [10240, 5120], P(('blk', 'uly')), may hold values from -8 to 8
- self_value: bfloat16 [10240, 5120], P(('blk', 'uly')), may hold values from -6 to 6
- cross_query: bfloat16 [10240, 5120], P(('blk', 'uly')), may hold values from -8 to 8
- text_key: bfloat16 [512, 5120], P('blk', 'uly'), may hold values from -8 to 8
- text_value: bfloat16 [512, 5120], P('blk', 'uly'), may hold values from -6 to 6
- padded_count: int32 [1], replicated, may hold values from 0 to 2560
Outputs:
- self_out: bfloat16 [10240, 5120], P(('blk', 'uly'))
- cross_out: bfloat16 [10240, 5120], P(('blk', 'uly'))
The draws below stay inside these ranges and needn't reach their ends.
All inputs are finite; a program needn't handle non-finite values.
Results may differ from the reference program's by a relative error of at most 0.0099.
Values may be sent and summed in bfloat16 or wider, within the bound.
A program may use at most 128 MiB of HBM per device.

```python
import math
import jax
import jax.numpy as jnp
from jax import lax

HEADS = 40
HD = 128
TEXT = 512
TH = 4
TW = 10
ROW_TILES = 8
FRAMES = 4
GRID_H = 32
GRID_W = 80
TOKENS = 10240
N_ULY = 8


def draw_self_query(key, part):
    own_key = jax.random.fold_in(key, 1)
    values = 1.8 * jax.random.truncated_normal(own_key, -4.0, 4.0, (TOKENS, HEADS * HD), jnp.float32)
    return values.astype(jnp.bfloat16)


def draw_self_key(key, part):
    own_key = jax.random.fold_in(key, 2)
    values = 1.8 * jax.random.truncated_normal(own_key, -4.0, 4.0, (TOKENS, HEADS * HD), jnp.float32)
    return values.astype(jnp.bfloat16)


def draw_cross_query(key, part):
    own_key = jax.random.fold_in(key, 3)
    values = 1.6 * jax.random.truncated_normal(own_key, -4.0, 4.0, (TOKENS, HEADS * HD), jnp.float32)
    return values.astype(jnp.bfloat16)


def draw_text_key(key, part):
    own_key = jax.random.fold_in(key, 4)
    values = 1.6 * jax.random.truncated_normal(own_key, -4.0, 4.0, (TEXT, HEADS * HD), jnp.float32)
    return values.astype(jnp.bfloat16)


def shard_levels(key, dims, cuts, smallest, top_value):
    gain, own = 1.0, jax.random.fold_in(key, 6)
    for dim, blocks in cuts:
        heights = jnp.exp(jax.random.uniform(jax.random.fold_in(own, dim), (blocks,), jnp.float32, smallest / len(cuts), top_value / len(cuts)))
        gain = gain * jnp.repeat(heights, dims[dim] // blocks).reshape([-1 if axis == dim else 1 for axis in range(len(dims))])
    return gain


def centred(key, shape, scale, reach, cuts=(), kind=jnp.bfloat16):
    values = scale * jax.random.normal(key, shape, jnp.float32)
    if cuts:
        values = values * shard_levels(key, shape, cuts, -0.22, 0.18)
    return jnp.clip(values, -reach, reach).astype(kind)


def setup_inputs(seed: int = 0) -> dict:
    keys = jax.random.split(jax.random.key(seed), 8)
    return {
        "self_query": draw_self_query(jax.random.fold_in(keys[7], 71), 0),
        "self_key": draw_self_key(jax.random.fold_in(keys[7], 71), 0),
        "self_value": centred(keys[2], (TOKENS, HEADS * HD), 1.0, 6.0, ((0, 256),)),
        "cross_query": draw_cross_query(jax.random.fold_in(keys[7], 71), 0),
        "text_key": draw_text_key(jax.random.fold_in(keys[7], 71), 0),
        "text_value": centred(keys[5], (TEXT, HEADS * HD), 1.0, 6.0, ((0, 32), (1, 8))),
        "padded_count": jax.random.randint(keys[6], (1,), 0, TOKENS // 4 + 1).astype(jnp.int32),
    }


neg_fill = -1e+30

def rope_tables(raster, head_size, grid_height, grid_width):
    frame_cells = grid_height * grid_width
    frame_index = raster // frame_cells
    row_index = raster // grid_width % grid_height
    col_index = raster % grid_width
    pair_index = lax.iota(jnp.int32, head_size) // 2
    side_pairs = head_size // 6
    first_pairs = head_size // 2 - 2 * side_pairs
    in_frames = pair_index < first_pairs
    in_rows = pair_index < first_pairs + side_pairs
    numerator = jnp.where(in_frames, pair_index, jnp.where(in_rows, pair_index - first_pairs, pair_index - first_pairs - side_pairs)).astype(jnp.float32)
    denominator = jnp.where(in_frames, first_pairs, side_pairs).astype(jnp.float32)
    omegas = jnp.power(jnp.float32(10000.0), -(numerator / denominator))
    position = jnp.where(in_frames[None, :], frame_index[:, None], jnp.where(in_rows[None, :], row_index[:, None], col_index[:, None])).astype(jnp.float32)
    angles = position * omegas[None, :]
    return (jnp.cos(angles), jnp.sin(angles))

def rotate(values, cosine_table, sine_table):
    channels = values.shape[1]
    repeats = channels // cosine_table.shape[1]
    widened = values.astype(jnp.float32)
    channel = lax.iota(jnp.int32, channels)
    partner = jnp.where(channel % 2 == 0, -jnp.roll(widened, -1, axis=1), jnp.roll(widened, 1, axis=1))
    return (widened * jnp.tile(cosine_table, (1, repeats)) + partner * jnp.tile(sine_table, (1, repeats))).astype(jnp.bfloat16)

def softmax_rows(query_block, key_rows, value_rows, key_mask, scaling):
    scores = jnp.dot(query_block, key_rows.T, preferred_element_type=jnp.float32) * scaling
    if key_mask is not None:
        scores = jnp.where(key_mask[None, :], scores, neg_fill)
    row_peak = lax.optimization_barrier(jnp.max(scores, axis=1, keepdims=True))
    weights = jnp.exp(scores - row_peak)
    totals = lax.optimization_barrier(jnp.sum(weights, axis=1, keepdims=True))
    weighted = jnp.dot(weights.astype(jnp.bfloat16), value_rows, preferred_element_type=jnp.float32)
    return (weighted / totals).astype(jnp.bfloat16)

def attention(queries, keys_all, values_all, key_mask, scaling):
    query_count = queries.shape[0]
    block_rows = 512 if query_count % 512 == 0 else query_count
    block_count = query_count // block_rows
    query_heads = queries.reshape(block_count, block_rows, HEADS, HD).transpose(2, 0, 1, 3)
    key_heads = keys_all.reshape(keys_all.shape[0], HEADS, HD).transpose(1, 0, 2)
    value_heads = values_all.reshape(values_all.shape[0], HEADS, HD).transpose(1, 0, 2)

    def one_head(head_index):

        def one_block(block_index):
            return softmax_rows(query_heads[head_index, block_index], key_heads[head_index], value_heads[head_index], key_mask, scaling)
        return lax.map(one_block, jnp.arange(block_count, dtype=jnp.int32))
    outputs = lax.map(one_head, jnp.arange(HEADS, dtype=jnp.int32))
    return outputs.transpose(1, 2, 0, 3).reshape(query_count, HEADS * HD)

def reference(self_query, self_key, self_value, cross_query, text_key, text_value, padded_count):
    channels = HEADS * HD

    def frame_major(array):
        tile_grid = array.reshape(FRAMES, ROW_TILES, N_ULY, TH, TW, channels)
        return tile_grid.transpose(0, 1, 3, 2, 4, 5).reshape(TOKENS, channels)
    query_rows = frame_major(self_query)
    key_rows = frame_major(self_key)
    value_rows = frame_major(self_value)
    cross_rows = frame_major(cross_query)
    raster = lax.iota(jnp.int32, TOKENS)
    cosine_table, sine_table = rope_tables(raster, HD, GRID_H, GRID_W)
    query_rot = rotate(query_rows, cosine_table, sine_table)
    key_rot = rotate(key_rows, cosine_table, sine_table)
    scaling = 1.0 / math.sqrt(HD)
    key_mask = raster < TOKENS - padded_count[0]
    self_out = attention(query_rot, key_rot, value_rows, key_mask, scaling)
    cross_out = attention(cross_rows, text_key, text_value, None, scaling)
    return (self_out, cross_out)
```

```python
import functools
import math

import jax
import jax.numpy as jnp
import numpy as np
from jax import lax
from jax.experimental import pallas as pl
from jax.experimental.pallas import tpu as pltpu
from jax.sharding import Mesh
from jax.sharding import PartitionSpec as P

HD = 128
TH = 4
TW = 10
TOK = TH * TW
ROW_TILES = 8
NX, NY, NZ, NC = 4, 4, 8, 2
LAYER = 5
HEADS = NZ * LAYER
GRID_H = TH * ROW_TILES
GRID_W = TW * NZ
KEYS = NX * NY * NZ * NC * TOK
LAST = KEYS // NX
PAD = 24
GROUPS = 16
ULY = ("uly_0", "uly_1")
BLK = ("blk_0", "blk_1", "blk_2")
NEG = -1e30
MESH = pl.DeviceIdType.MESH


def place():
    x = lax.axis_index("blk_0")
    y = lax.axis_index("blk_1")
    z = lax.axis_index("uly_0") * 2 + lax.axis_index("blk_2")
    return x, y, z, lax.axis_index("uly_1")


def at_xz(x, z):
    return {"blk_0": x, "uly_0": z // 2, "blk_2": lax.rem(z, 2)}


def prep_kernel(cos_ref, sin_ref, q_ref, k_ref, v_ref, c_ref, qo, ko, vo, co):
    cos = cos_ref[...]
    sin = sin_ref[...]
    even = lax.rem(lax.broadcasted_iota(jnp.int32, (TOK, HD), 1), 2) == 0
    for h in range(LAYER):
        cut = slice(h * HD, (h + 1) * HD)
        for src, dst in ((q_ref, qo), (k_ref, ko)):
            wide = src[:, cut].astype(jnp.float32)
            swapped = jnp.where(even, pltpu.roll(wide, HD - 1, 1), pltpu.roll(wide, 1, 1))
            dst[h] = (wide * cos + swapped * sin).astype(jnp.bfloat16)
        vo[h] = v_ref[:, cut]
        co[h] = c_ref[:, cut]


def prep(cos, sin, arrays):
    table = pl.BlockSpec((TOK, HD), lambda i: (0, 0))
    wide = pl.BlockSpec((TOK, LAYER * HD), lambda i: (0, i))
    heads = pl.BlockSpec((LAYER, TOK, HD), lambda i: (i, 0, 0))
    return pl.pallas_call(
        prep_kernel,
        grid=(NZ,),
        in_specs=[table, table] + [wide] * 4,
        out_specs=[heads] * 4,
        out_shape=[jax.ShapeDtypeStruct((HEADS, TOK, HD), jnp.bfloat16)] * 4,
        name="prep",
    )(cos, sin, *arrays)


def gather_kernel(q, c, k, v, qa, ca, qb, cb, ka, va, kb, vb, send, recv, ring_send, ring_recv, twin_send, twin_recv):
    x, y, z, core = place()
    twin = {"uly_1": 1 - core}
    yp, ym, yo = lax.rem(y + 1, NY), lax.rem(y + NY - 1, NY), lax.rem(y + 2, NY)
    xp, xm, xo = lax.rem(x + 1, NX), lax.rem(x + NX - 1, NX), lax.rem(x + 2, NX)

    barrier = pltpu.get_barrier_semaphore()

    def greet(n, carry):
        peer = at_xz(lax.rem(x + n // NZ, NX), lax.rem(z + lax.rem(n, NZ), NZ))
        pl.semaphore_signal(barrier, inc=1, device_id=peer, device_id_type=MESH)
        return carry

    lax.fori_loop(1, NX * NZ, greet, 0)
    for peer in ({"blk_1": yp}, {"blk_1": ym}, twin):
        pl.semaphore_signal(barrier, inc=1, device_id=peer, device_id_type=MESH)
    pl.semaphore_wait(barrier, NX * NZ - 1 + 3)

    own_a, own_b = z * LAYER + x, z * LAYER + LAYER - 1
    pltpu.make_async_copy(q.at[own_b], qb.at[z], recv.at[0]).start()
    pltpu.make_async_copy(c.at[own_b], cb.at[z], recv.at[1]).start()
    pltpu.make_async_copy(k.at[own_b], kb.at[x, core, y, z], recv.at[2]).start()
    pltpu.make_async_copy(v.at[own_b], vb.at[x, core, y, z], recv.at[3]).start()
    pltpu.make_async_copy(q.at[own_a], qa.at[x, z], recv.at[4]).start()
    pltpu.make_async_copy(c.at[own_a], ca.at[x, z], recv.at[5]).start()
    pltpu.make_async_copy(k.at[own_a], ka.at[x, core, y, z], recv.at[6]).start()
    pltpu.make_async_copy(v.at[own_a], va.at[x, core, y, z], recv.at[7]).start()

    def push(src, dst, s, r, peer):
        pltpu.make_async_remote_copy(src, dst, send.at[s], recv.at[r], device_id=peer, device_id_type=MESH).start()

    def send_b(n, carry):
        tz = lax.rem(z + n, NZ)
        h, peer = tz * LAYER + LAYER - 1, at_xz(x, tz)
        push(k.at[h], kb.at[x, core, y, z], 2, 2, peer)
        push(v.at[h], vb.at[x, core, y, z], 3, 3, peer)
        return carry

    def send_a(n, carry):
        tx, tz = lax.rem(x + n // NZ, NX), lax.rem(z + lax.rem(n, NZ), NZ)
        h, peer = tz * LAYER + tx, at_xz(tx, tz)
        push(k.at[h], ka.at[x, core, y, z], 2, 6, peer)
        push(v.at[h], va.at[x, core, y, z], 3, 7, peer)
        return carry

    def send_qb(n, carry):
        tz = lax.rem(z + n, NZ)
        h, peer = tz * LAYER + LAYER - 1, at_xz(x, tz)
        push(q.at[h], qb.at[z], 0, 0, peer)
        push(c.at[h], cb.at[z], 1, 1, peer)
        return carry

    def send_qa(n, carry):
        tx, tz = lax.rem(x + n // NZ, NX), lax.rem(z + lax.rem(n, NZ), NZ)
        h, peer = tz * LAYER + tx, at_xz(tx, tz)
        push(q.at[h], qa.at[x, z], 0, 4, peer)
        push(c.at[h], ca.at[x, z], 1, 5, peer)
        return carry

    lax.fori_loop(1, NZ, send_b, 0)
    lax.fori_loop(1, NX * NZ, send_a, 0)
    lax.fori_loop(1, NZ, send_qb, 0)
    lax.fori_loop(1, NX * NZ, send_qa, 0)

    def arrived(ref, sem):
        pltpu.make_async_copy(ref, ref, sem).wait()

    def give(kind, region, axis, target, slot):
        for t, arr in enumerate(kind):
            pltpu.make_async_remote_copy(
                region(arr), region(arr), ring_send.at[slot, t], ring_recv.at[slot, t],
                device_id={axis: target}, device_id_type=MESH).start()

    def took(kind, region, slot):
        for t, arr in enumerate(kind):
            arrived(region(arr), ring_recv.at[slot, t])

    def share(kind, region, slot):
        for t, arr in enumerate(kind):
            pltpu.make_async_remote_copy(
                region(arr), region(arr), twin_send.at[slot, t], twin_recv.at[slot, t],
                device_id=twin, device_id_type=MESH).start()

    b, a = (kb, vb), (ka, va)
    b_y = lambda yy: lambda r: r.at[x, core, yy]
    b_half = lambda yy, s: lambda r: r.at[x, core, yy, pl.ds(4 * s, 4)]
    a_y = lambda yy: lambda r: r.at[:, core, yy]
    a_half = lambda yy, s: lambda r: r.at[pl.ds(2 * s, 2), core, yy]
    b_x = lambda xx: lambda r: r.at[xx, core]
    bx_half = lambda xx, s: lambda r: r.at[xx, core, pl.ds(2 * s, 2)]

    for t in range(2):
        arrived(b_y(y)(b[t]), recv.at[2 + t])
    give(b, b_y(y), "blk_1", yp, 0)
    give(b, b_y(y), "blk_1", ym, 1)
    for t in range(2):
        arrived(a_y(y)(a[t]), recv.at[6 + t])
    give(a, a_y(y), "blk_1", yp, 4)
    give(a, a_y(y), "blk_1", ym, 5)
    share(a, a_y(y), 0)
    took(b, b_y(ym), 0)
    give(b, b_half(ym, 0), "blk_1", yp, 2)
    took(b, b_y(yp), 1)
    give(b, b_half(yp, 1), "blk_1", ym, 3)
    took(b, b_half(yo, 0), 2)
    took(b, b_half(yo, 1), 3)
    give(b, b_x(x), "blk_0", xp, 8)
    give(b, b_x(x), "blk_0", xm, 9)
    share(b, b_x(x), 4)
    took(a, a_y(ym), 4)
    give(a, a_half(ym, 0), "blk_1", yp, 6)
    share(a, a_y(ym), 1)
    took(a, a_y(yp), 5)
    give(a, a_half(yp, 1), "blk_1", ym, 7)
    share(a, a_y(yp), 2)
    took(b, b_x(xm), 8)
    give(b, bx_half(xm, 0), "blk_0", xp, 10)
    share(b, b_x(xm), 5)
    took(b, b_x(xp), 9)
    give(b, bx_half(xp, 1), "blk_0", xm, 11)
    share(b, b_x(xp), 6)
    took(a, a_half(yo, 0), 6)
    took(a, a_half(yo, 1), 7)
    share(a, a_y(yo), 3)
    took(b, bx_half(xo, 0), 10)
    took(b, bx_half(xo, 1), 11)
    share(b, b_x(xo), 7)

    arrived(qb, recv.at[0])
    arrived(cb, recv.at[1])
    arrived(qa, recv.at[4])
    arrived(ca, recv.at[5])
    other = 1 - core
    for slot in range(4):
        for t in range(2):
            yy = (y, ym, yp, yo)[slot]
            arrived(a[t].at[:, other, yy], twin_recv.at[slot, t])
            xx = (x, xm, xp, xo)[slot]
            arrived(b[t].at[xx, other], twin_recv.at[4 + slot, t])
    for s, ref in enumerate((q, c, k, v)):
        arrived(ref.at[pl.ds(0, NX * NZ - 1 + NZ - 1)], send.at[s])
    for t in range(2):
        for slot in (0, 1):
            arrived(b_y(y)(b[t]), ring_send.at[slot, t])
            arrived(a_y(y)(a[t]), ring_send.at[4 + slot, t])
            arrived(b_x(x)(b[t]), ring_send.at[8 + slot, t])
            arrived(b_half(y, slot)(b[t]), ring_send.at[2 + slot, t])
            arrived(a_half(y, slot)(a[t]), ring_send.at[6 + slot, t])
            arrived(bx_half(x, slot)(b[t]), ring_send.at[10 + slot, t])
        for slot in range(4):
            arrived(a_y(y)(a[t]), twin_send.at[slot, t])
            arrived(b_x(x)(b[t]), twin_send.at[4 + slot, t])


def gather(q, c, k, v):
    any_spec = pl.BlockSpec(memory_space=pl.ANY)
    shapes = [(NX, NZ)] * 2 + [(NZ,)] * 2 + [(NX, NC, NY, NZ)] * 4
    dma = pltpu.SemaphoreType.DMA
    return pl.pallas_call(
        gather_kernel,
        in_specs=[any_spec] * 4,
        out_specs=[any_spec] * 8,
        out_shape=[jax.ShapeDtypeStruct((*s, TOK, HD), jnp.bfloat16) for s in shapes],
        scratch_shapes=[dma((4,)), dma((8,)), dma((12, 2)), dma((12, 2)), dma((8, 2)), dma((8, 2))],
        compiler_params=pltpu.CompilerParams(collective_id=0, has_side_effects=True),
        name="gather",
    )(q, c, k, v)


def attend_kernel(scaling, block, blocks, masked, rows, *refs):
    if masked:
        q_ref, k_ref, v_ref, perm_ref, bias_ref, o_ref, vt, s0, s1, ot = refs
    else:
        q_ref, k_ref, v_ref, perm_ref, o_ref, vt, s0, s1, ot = refs
        bias_ref = None
    step = pl.program_id(0)
    steps = pl.num_programs(0)
    scale = scaling * math.log2(math.e)
    q = q_ref[...]

    @pl.when(step == 0)
    def _():
        @pl.loop(0, blocks)
        def _(j):
            cut = pl.ds(pl.multiple_of(j * block, block), block)
            vt[:, cut] = v_ref[cut, :].T

    def scores(j, into, with_bias):
        start = pl.multiple_of(j * block, block)
        s = lax.dot_general(k_ref[pl.ds(start, block), :], q, (((1,), (1,)), ((), ())),
                            preferred_element_type=jnp.float32)
        if with_bias:
            off = pl.multiple_of((j - (blocks - masked)) * block, block)
            bias = bias_ref[pl.ds(off, block), 0:1]
            s = s + bias
        into[...] = s
        return jnp.max(s, axis=0, keepdims=True)

    def absorb(j, held, peak, state):
        m, l, acc = state
        start = pl.multiple_of(j * block, block)
        new = jnp.maximum(m, peak)
        shrink = jnp.exp2((m - new) * scale)
        p = jnp.exp2((held[...] - new) * scale)
        l = l * shrink + jnp.sum(p, axis=0, keepdims=True)
        acc = acc * shrink + jnp.dot(vt[:, pl.ds(start, block)], p.astype(jnp.bfloat16),
                                     preferred_element_type=jnp.float32)
        return new, l, acc

    state = (jnp.full((1, rows), NEG, jnp.float32), jnp.zeros((1, rows), jnp.float32),
             jnp.zeros((HD, rows), jnp.float32))
    plain = blocks - masked
    first = scores(0, s0, False)

    def pair(bias_1, bias_0):
        def run(i, carry):
            peak, state = carry
            j = i * 2
            peak_1 = scores(j + 1, s1, bias_1)
            state = absorb(j, s0, peak, state)
            peak = scores(jnp.minimum(j + 2, blocks - 1), s0, bias_0)
            state = absorb(j + 1, s1, peak_1, state)
            return peak, state
        return run

    carry = (first, state)
    if masked:
        carry = lax.fori_loop(0, plain // 2 - 1, pair(False, False), carry)
        carry = lax.fori_loop(plain // 2 - 1, plain // 2, pair(False, True), carry)
        carry = lax.fori_loop(plain // 2, blocks // 2, pair(True, True), carry)
    else:
        carry = lax.fori_loop(0, blocks // 2, pair(False, False), carry)
    m, l, acc = carry[1]
    out_t = (acc / l).astype(jnp.bfloat16)
    ot[:, pl.ds(pl.multiple_of(step * rows, 128), rows)] = out_t

    @pl.when(step == steps - 1)
    def _():
        for n in range(o_ref.shape[0]):
            o_ref[n] = lax.dot_general(
                perm_ref[...], ot[:, n * NZ * TOK : (n + 1) * NZ * TOK], (((1,), (1,)), ((), ())),
                preferred_element_type=jnp.float32).astype(jnp.bfloat16)


def attend(q, k, v, perm, bias, rows, block, scaling, name):
    total, keys = q.shape[0], k.shape[0]
    blocks = keys // block
    masked = 0 if bias is None else LAST // block
    outs = total // (NZ * TOK)
    whole = lambda a: pl.BlockSpec(a.shape, lambda i: (0,) * a.ndim)
    args = [q, k, v, perm] + ([] if bias is None else [bias])
    return pl.pallas_call(
        functools.partial(attend_kernel, scaling, block, blocks, masked, rows),
        grid=(total // rows,),
        in_specs=[pl.BlockSpec((rows, HD), lambda i: (i, 0))] + [whole(a) for a in args[1:]],
        out_specs=pl.BlockSpec((outs, GROUPS * PAD, HD), lambda i: (0, 0, 0)),
        out_shape=jax.ShapeDtypeStruct((outs, GROUPS * PAD, HD), jnp.bfloat16),
        scratch_shapes=[
            pltpu.VMEM((HD, keys), jnp.bfloat16),
            pltpu.VMEM((block, rows), jnp.float32),
            pltpu.VMEM((block, rows), jnp.float32),
            pltpu.VMEM((HD, total), jnp.bfloat16),
        ],
        cost_estimate=pl.CostEstimate(flops=4 * total * keys * HD, bytes_accessed=4 * keys * HD,
                                      transcendentals=total * keys),
        name=name,
    )(*args)


def order_matrix():
    perm = np.zeros((GROUPS * PAD, NZ * TOK), np.float32)
    for zl in range(2):
        for a in range(2):
            for i in range(TH):
                for zh2 in range(2):
                    for j in range(TW):
                        row = (zl * 8 + a * 4 + i) * PAD + zh2 * TW + j
                        perm[row, (2 * (2 * a + zh2) + zl) * TOK + i * TW + j] = 1
    return jnp.asarray(perm, jnp.bfloat16)


def deliver_kernel(sa, ca, sb, cb, rs, rc, send, recv, near):
    x, y, z, core = place()
    zl, zh = lax.axis_index("blk_2"), lax.axis_index("uly_0")
    barrier = pltpu.get_barrier_semaphore()
    count = NX * NZ * NC

    def target(n):
        tx = lax.rem(x + n // (NZ * NC), NX)
        rest = lax.rem(n, NZ * NC)
        ti = lax.rem(zh + rest // 4, 4)
        tl = lax.rem(zl + lax.rem(rest // 2, 2), 2)
        ta = lax.rem(core + lax.rem(rest, 2), 2)
        return tx, ti, tl, ta, {"blk_0": tx, "uly_0": ti, "blk_2": tl, "uly_1": ta}

    def greet(n, carry):
        pl.semaphore_signal(barrier, inc=1, device_id=target(n)[-1], device_id_type=MESH)
        return carry

    lax.fori_loop(1, count, greet, 0)
    pl.semaphore_wait(barrier, count - 1)

    head_a, head_b = z * LAYER + x, z * LAYER + LAYER - 1
    own = zl * 8 + core * 4 + zh
    for n, (a, b, r) in enumerate(((sa, sb, rs), (ca, cb, rc))):
        pltpu.make_async_copy(a.at[x, own], r.at[head_a, core], near.at[n, 0]).start()
        pltpu.make_async_copy(b.at[own], r.at[head_b, core], near.at[n, 1]).start()

    def push(src, dst, n, peer):
        pltpu.make_async_remote_copy(src, dst, send.at[n], recv.at[n], device_id=peer, device_id_type=MESH).start()

    def send_b(n, carry):
        tx, ti, tl, ta, peer = target(n)
        g = tl * 8 + ta * 4 + ti
        push(sb.at[g], rs.at[head_b, core], 0, peer)
        push(cb.at[g], rc.at[head_b, core], 1, peer)
        return carry

    def send_a(n, carry):
        tx, ti, tl, ta, peer = target(n)
        g = tl * 8 + ta * 4 + ti
        push(sa.at[tx, g], rs.at[head_a, core], 0, peer)
        push(ca.at[tx, g], rc.at[head_a, core], 1, peer)
        return carry

    lax.fori_loop(1, NZ * NC, send_b, 0)
    lax.fori_loop(1, count, send_a, 0)

    def arrived(ref, sem):
        pltpu.make_async_copy(ref, ref, sem).wait()

    for n, (a, b, r) in enumerate(((sa, sb, rs), (ca, cb, rc))):
        arrived(r.at[head_a, core], near.at[n, 0])
        arrived(r.at[head_b, core], near.at[n, 1])
        moved = r.at[pl.ds(0, (count - 1 + NZ * NC - 1) // 2)]
        arrived(moved, recv.at[n])
        arrived(moved, send.at[n])


def deliver(sa, ca, sb, cb):
    any_spec = pl.BlockSpec(memory_space=pl.ANY)
    dma = pltpu.SemaphoreType.DMA
    return pl.pallas_call(
        deliver_kernel,
        in_specs=[any_spec] * 4,
        out_specs=[any_spec] * 2,
        out_shape=[jax.ShapeDtypeStruct((HEADS, NC, PAD, HD), jnp.bfloat16)] * 2,
        scratch_shapes=[dma((2,)), dma((2,)), dma((2, 2))],
        compiler_params=pltpu.CompilerParams(collective_id=1, has_side_effects=True),
        name="deliver",
    )(sa, ca, sb, cb)


def rope_tables(frame, row, col):
    pair = lax.iota(jnp.int32, HD) // 2
    side = HD // 6
    first = HD // 2 - 2 * side
    in_frames = pair < first
    in_rows = pair < first + side
    numerator = jnp.where(in_frames, pair, jnp.where(in_rows, pair - first, pair - first - side)).astype(jnp.float32)
    denominator = jnp.where(in_frames, first, side).astype(jnp.float32)
    omegas = jnp.power(jnp.float32(10000.0), -(numerator / denominator))
    position = jnp.where(in_frames[None, :], frame[:, None],
                         jnp.where(in_rows[None, :], row[:, None], col[:, None])).astype(jnp.float32)
    angles = position * omegas[None, :]
    sign = jnp.where(lax.iota(jnp.int32, HD) % 2 == 0, -1.0, 1.0)
    return jnp.cos(angles), jnp.sin(angles) * sign[None, :]


def body(self_query, self_key, self_value, cross_query, text_key, text_value, padded_count):
    scaling = 1.0 / math.sqrt(HD)
    x, y, z, core = place()
    zl, zh = lax.axis_index("blk_2"), lax.axis_index("uly_0")

    rows = text_key.shape[0]
    text = jnp.stack([text_key, text_value]).reshape(2, rows, LAYER, HD).transpose(0, 2, 1, 3)
    text = lax.ppermute(text, ("blk_2", "uly_1"), [(0, 0), (1, 2), (2, 1), (3, 3)])
    text = lax.all_gather(text, ("blk_0", "blk_1", "uly_1"), axis=2, tiled=True)

    token = lax.iota(jnp.int32, TOK)
    block = (x * NY + y) * 2 + zl
    row = lax.rem(block, ROW_TILES) * TH + token // TW
    col = (zh * 2 + core) * TW + token % TW
    cos, sin = rope_tables(jnp.full((TOK,), block // ROW_TILES), row, col)
    qh, kh, vh, ch = prep(cos, sin, (self_query, self_key, self_value, cross_query))

    qa, ca, qb, cb, ka, va, kb, vb = gather(qh, ch, kh, vh)

    order = lax.iota(jnp.int32, LAST)
    n_t, n_z, n_y, n_c = order % TOK, order // TOK % NZ, order // (TOK * NZ) % NY, order // (TOK * NZ * NY)
    n_row = (n_y * 2 + n_z % 2) * TH + n_t // TW
    n_col = (n_z // 2 * 2 + n_c) * TW + n_t % TW
    index = (NX - 1) * GRID_H * GRID_W + n_row * GRID_W + n_col
    bias = jnp.where(index < KEYS - padded_count[0], 0.0, NEG).astype(jnp.float32)
    bias = jnp.broadcast_to(bias[:, None], (LAST, HD))

    perm = order_matrix()
    flat = lambda t: t.reshape(-1, HD)
    text_a = lax.dynamic_index_in_dim(text, x, 1, keepdims=False)
    cross_a = attend(flat(ca), text_a[0], text_a[1], perm, None, 256, 256, scaling, "cross_a")
    cross_b = attend(flat(cb), text[0, LAYER - 1], text[1, LAYER - 1], perm, None, NZ * TOK, 256, scaling, "cross_b")
    self_a = attend(flat(qa), flat(ka), flat(va), perm, bias, 256, 1280, scaling, "self_a")
    self_b = attend(flat(qb), flat(kb), flat(vb), perm, bias, NZ * TOK, 1280, scaling, "self_b")

    split_a = lambda o: o.reshape(NX, GROUPS, PAD, HD)
    split_b = lambda o: o.reshape(GROUPS, PAD, HD)
    results = deliver(split_a(self_a), split_a(cross_a), split_b(self_b), split_b(cross_b))

    def finish(r):
        r = r[:, :, : 2 * TW].reshape(HEADS, NC, 2, TW, HD)
        return r.transpose(2, 1, 3, 0, 4).reshape(TOK, HEADS * HD)

    return finish(results[0]), finish(results[1])


def solution(mesh):
    split = Mesh(mesh.devices.reshape(4, 4, 2, 4, 2), BLK + ULY)
    own = P(BLK + ULY, None)
    return jax.shard_map(body, mesh=split, in_specs=(own,) * 4 + (P(BLK, ULY),) * 2 + (P(),),
                         out_specs=(own, own), check_vma=False)
```

```python
import functools
import math

import jax
import jax.numpy as jnp
import numpy as np
from jax import lax
from jax.experimental import pallas as pl
from jax.experimental.pallas import tpu as pltpu
from jax.sharding import Mesh
from jax.sharding import PartitionSpec as P

HD = 128
TH = 4
TW = 10
TOK = TH * TW
ROW_TILES = 8
NX, NY, NZ, NC = 4, 4, 8, 2
LAYER = 5
HEADS = NZ * LAYER
GRID_H = TH * ROW_TILES
GRID_W = TW * NZ
KEYS = NX * NY * NZ * NC * TOK
LAST = KEYS // NX
PAD = 24
GROUPS = 16
ULY = ("uly_0", "uly_1")
BLK = ("blk_0", "blk_1", "blk_2")
NEG = -1e30
MESH = pl.DeviceIdType.MESH


def place():
    x = lax.axis_index("blk_0")
    y = lax.axis_index("blk_1")
    z = lax.axis_index("uly_0") * 2 + lax.axis_index("blk_2")
    return x, y, z, lax.axis_index("uly_1")


def at_xz(x, z):
    return {"blk_0": x, "uly_0": z // 2, "blk_2": lax.rem(z, 2)}


def prep_kernel(cos_ref, sin_ref, q_ref, k_ref, v_ref, c_ref, qo, ko, vo, co):
    cos = cos_ref[...]
    sin = sin_ref[...]
    even = lax.rem(lax.broadcasted_iota(jnp.int32, (TOK, HD), 1), 2) == 0
    for h in range(LAYER):
        cut = slice(h * HD, (h + 1) * HD)
        for src, dst in ((q_ref, qo), (k_ref, ko)):
            wide = src[:, cut].astype(jnp.float32)
            swapped = jnp.where(even, pltpu.roll(wide, HD - 1, 1), pltpu.roll(wide, 1, 1))
            dst[h] = (wide * cos + swapped * sin).astype(jnp.bfloat16)
        vo[h] = v_ref[:, cut]
        co[h] = c_ref[:, cut]


def prep(cos, sin, arrays):
    table = pl.BlockSpec((TOK, HD), lambda i: (0, 0))
    wide = pl.BlockSpec((TOK, LAYER * HD), lambda i: (0, i))
    heads = pl.BlockSpec((LAYER, TOK, HD), lambda i: (i, 0, 0))
    return pl.pallas_call(
        prep_kernel,
        grid=(NZ,),
        in_specs=[table, table] + [wide] * 4,
        out_specs=[heads] * 4,
        out_shape=[jax.ShapeDtypeStruct((HEADS, TOK, HD), jnp.bfloat16)] * 4,
        name="prep",
    )(cos, sin, *arrays)


SPAN = NZ * TOK
REGION = NX * SPAN
WIDE = 384
TILE = 256
SCALE = math.log2(math.e) / math.sqrt(HD)
NT = (((1,), (1,)), ((), ()))


def block_kernel(
    q, c, k, v, text, bias_a, bias_b, perm,
    rs, rc, qa_h, ca_h, qb_h, cb_h, ka_h, va_h, kb_h, vb_h,
    qa, qb, ca, cb, ka, va, kb, vb, txt, s0, s1, vt, acc, row_m, row_l, ot, oa, ob, oc, od, part, stat,
    send, recv, local, ring_send, ring_recv, twin_send, twin_recv, fan_send, fan_recv, part_send, part_recv,
    text_send, text_recv, out_send, out_recv, near,
):
    x, y, z, core = place()
    zl, zh = lax.axis_index("blk_2"), lax.axis_index("uly_0")
    twin = {"uly_1": 1 - core}
    yp, ym, yo = lax.rem(y + 1, NY), lax.rem(y + NY - 1, NY), lax.rem(y + 2, NY)
    others = NX * NZ * NC - 1

    def owner(n, m):
        ti = lax.rem(zh + m // 4, 4)
        tl = lax.rem(zl + lax.rem(m // 2, 2), 2)
        ta = lax.rem(core + lax.rem(m, 2), 2)
        peer = {"blk_0": lax.rem(x + n, NX), "uly_0": ti, "blk_2": tl, "uly_1": ta}
        return tl * 8 + ta * 4 + ti, peer

    barrier = pltpu.get_barrier_semaphore()

    def greet(n, carry):
        peer = owner(n // GROUPS, lax.rem(n, GROUPS))[1]
        pl.semaphore_signal(barrier, inc=1, device_id=peer, device_id_type=MESH)
        return carry

    lax.fori_loop(1, others + 1, greet, 0)
    for yy in (yp, ym, yo):
        pl.semaphore_signal(barrier, inc=1, device_id={"blk_1": yy}, device_id_type=MESH)
    pl.semaphore_wait(barrier, others + 3)

    def arrived(ref, sem):
        pltpu.make_async_copy(ref, ref, sem).wait()

    def push(src, dst, s, r, peer):
        pltpu.make_async_remote_copy(src, dst, s, r, device_id=peer, device_id_type=MESH).start()

    own_a, own_b = z * LAYER + x, z * LAYER + LAYER - 1

    def rows(ref, start):
        return ref.at[pl.ds(pl.multiple_of(start, 8), TOK)]

    def rows_of(n):
        return n * SPAN + z * TOK

    def send_b(pairs):
        def run(n, carry):
            tz = lax.rem(z + n, NZ)
            h, peer = tz * LAYER + LAYER - 1, at_xz(x, tz)
            for s, src, r, dst in pairs:
                push(src.at[h], rows(dst, z * TOK), send.at[s], recv.at[r], peer)
            return carry
        for s, src, r, dst in pairs:
            pltpu.make_async_copy(src.at[own_b], rows(dst, z * TOK), recv.at[r]).start()
        lax.fori_loop(1, NZ, run, 0)

    def send_a(pairs, relative):
        def where(tx):
            return rows_of(lax.rem(x - tx + NX, NX)) if relative else rows_of(x)
        def run(n, carry):
            tx, tz = lax.rem(x + n // NZ, NX), lax.rem(z + lax.rem(n, NZ), NZ)
            h, peer = tz * LAYER + tx, at_xz(tx, tz)
            for s, src, r, dst in pairs:
                push(src.at[h], rows(dst, where(tx)), send.at[s], recv.at[r], peer)
            return carry
        for s, src, r, dst in pairs:
            pltpu.make_async_copy(src.at[own_a], rows(dst, where(x)), recv.at[r]).start()
        lax.fori_loop(1, NX * NZ, run, 0)

    send_b(((2, k, 0, kb_h), (3, v, 1, vb_h), (0, q, 2, qb_h)))
    for n in range(1, NX):
        tx = lax.rem(x + n, NX)
        for ab, h in ((0, tx), (1, LAYER - 1)):
            push(text.at[h], txt.at[core, y, x, ab], text_send.at[0], text_recv.at[0], {"blk_0": tx})
    for ab, h in ((0, x), (1, LAYER - 1)):
        pltpu.make_async_copy(text.at[h], txt.at[core, y, x, ab], local.at[8 + ab]).start()
    send_a(((2, k, 3, ka_h), (3, v, 4, va_h)), False)
    send_a(((0, q, 5, qa_h),), True)
    send_b(((1, c, 6, cb_h),))
    send_a(((1, c, 7, ca_h),), True)

    qb[:, SPAN:, :] = jnp.zeros((NX, WIDE - SPAN, HD), jnp.bfloat16)
    cb[SPAN:, :] = jnp.zeros((WIDE - SPAN, HD), jnp.bfloat16)
    row_m[...] = jnp.full_like(row_m, NEG)
    row_l[...] = jnp.zeros_like(row_l)
    acc[...] = jnp.zeros_like(acc)
    stat[...] = jnp.zeros_like(stat)

    def give(kind, region, target, n):
        for t, arr in enumerate(kind):
            push(region(arr), region(arr), ring_send.at[n, t], ring_recv.at[n, t], {"blk_1": target})

    def took(kind, region, n):
        for t, arr in enumerate(kind):
            arrived(region(arr), ring_recv.at[n, t])

    def share(kind, region, n):
        for t, arr in enumerate(kind):
            push(region(arr), region(arr), twin_send.at[n, t], twin_recv.at[n, t], twin)

    def land(src, dst, r, n):
        arrived(src, recv.at[r])
        pltpu.make_async_copy(src, dst, local.at[n]).start()
        return lambda: pltpu.make_async_copy(src, dst, local.at[n]).wait()

    a, b = (ka, va), (kb, vb)
    mine = core * NY
    a_y = lambda yy: lambda r: r.at[mine + yy]
    a_half = lambda yy, s: lambda r: r.at[mine + yy, pl.ds(s * (REGION // 2), REGION // 2)]
    b_y = lambda yy: lambda r: r.at[core, yy]
    b_half = lambda yy, s: lambda r: r.at[core, yy, pl.ds(s * (SPAN // 2), SPAN // 2)]
    b_all = lambda r: r.at[core]

    for done in [land(kb_h, kb.at[core, y], 0, 0), land(vb_h, vb.at[core, y], 1, 1)]:
        done()
    give(b, b_y(y), yp, 0)
    give(b, b_y(y), ym, 1)
    land(qb_h, qb.at[0, pl.ds(0, SPAN)], 2, 2)()
    for n in range(1, NX):
        push(qb.at[0, pl.ds(0, SPAN)], qb.at[NX - n, pl.ds(0, SPAN)], fan_send.at[n - 1], fan_recv.at[NX - n - 1],
             {"blk_0": lax.rem(x + n, NX)})
    arrived(txt.at[core, y, pl.ds(0, NX - 1)], text_recv.at[0])
    for ab in range(2):
        arrived(txt.at[core, y, x, ab], local.at[8 + ab])
    for yy in (yp, ym, yo):
        push(txt.at[core, y], txt.at[core, y], text_send.at[1], text_recv.at[1], {"blk_1": yy})
    took(b, b_y(ym), 0)
    give(b, b_half(ym, 0), yp, 2)
    took(b, b_y(yp), 1)
    give(b, b_half(yp, 1), ym, 3)
    took(b, b_half(yo, 0), 2)
    took(b, b_half(yo, 1), 3)
    share(b, b_all, 4)
    arrived(txt.at[core, pl.ds(0, NY - 1)], text_recv.at[1])
    push(txt.at[core], txt.at[core], text_send.at[2], text_recv.at[2], twin)
    for n in range(1, NX):
        arrived(qb.at[n, pl.ds(0, SPAN)], fan_recv.at[n - 1])

    held = (s0, s1)

    def absorb(cols, width, s, peak):
        m = row_m[0:1, cols]
        new = jnp.maximum(m, peak)
        shrink = jnp.exp2((m - new) * SCALE)
        p = jnp.exp2((s[:, :width] - new) * SCALE)
        row_m[0:1, cols] = new
        row_l[0:1, cols] = row_l[0:1, cols] * shrink + jnp.sum(p, axis=0, keepdims=True)
        acc[:, cols] = acc[:, cols] * shrink + jnp.dot(
            vt[...], p.astype(jnp.bfloat16), preferred_element_type=jnp.float32)

    def attend(queries, width, scores):
        peaks = scores(queries[0][0], s0)
        for n, (_, cols) in enumerate(queries):
            ahead = scores(queries[n + 1][0], held[(n + 1) % 2]) if n + 1 < len(queries) else None
            absorb(cols, width, held[n % 2], peaks)
            peaks = ahead

    def over(bias, width):
        return jnp.concatenate([bias] * (width // HD), axis=1)

    b_tiles = [(n, slice(n * WIDE, (n + 1) * WIDE)) for n in range(NX)]

    def b_region(i, carry):
        cc = lax.rem(core + i, NC)

        @pl.when(i == 1)
        def _():
            for t in range(2):
                arrived(b[t].at[1 - core], twin_recv.at[4, t])

        vt[...] = vb[cc].reshape(REGION, HD).T

        def scores(n, into):
            s = lax.dot_general(kb[cc].reshape(REGION, HD), qb[n], NT, preferred_element_type=jnp.float32)
            s = s + over(bias_b[pl.ds(pl.multiple_of(cc * REGION, 8), REGION), :], WIDE)
            into[...] = s
            return jnp.max(s, axis=0, keepdims=True)

        attend(b_tiles, WIDE, scores)
        return carry

    lax.fori_loop(0, NC, b_region, 0)
    for n in range(NX):
        cols = slice(n * WIDE, (n + 1) * WIDE)
        part[n] = (acc[:, cols] / row_l[0:1, cols]).astype(jnp.bfloat16)
        stat[n, 0:1, :] = row_m[0:1, cols]
        stat[n, 1:2, :] = row_l[0:1, cols]
    for n in range(1, NX):
        peer = {"blk_0": lax.rem(x + n, NX)}
        push(part.at[n], part.at[NX + n], part_send.at[n - 1, 0], part_recv.at[n - 1, 0], peer)
        push(stat.at[n], stat.at[NX + n], part_send.at[n - 1, 1], part_recv.at[n - 1, 1], peer)

    row_m[...] = jnp.full_like(row_m, NEG)
    row_l[...] = jnp.zeros_like(row_l)
    acc[...] = jnp.zeros_like(acc)

    for done in [land(ka_h, ka.at[mine + y], 3, 3), land(va_h, va.at[mine + y], 4, 4)]:
        done()
    give(a, a_y(y), yp, 4)
    give(a, a_y(y), ym, 5)
    share(a, a_y(y), 0)

    def ordered(cols):
        return lax.dot_general(perm[...], cols, NT, preferred_element_type=jnp.float32).reshape(
            GROUPS, PAD, HD).astype(jnp.bfloat16)

    def deliver(src, result, n, head, which):
        def run(m, carry):
            g, peer = owner(n, m)
            push(src.at[g], result.at[head, core], out_send.at[which], out_recv.at[which], peer)
            return carry
        lax.fori_loop(1 if n == 0 else 0, GROUPS, run, 0)

    def keep(src, result, head, n):
        return pltpu.make_async_copy(src.at[zl * 8 + core * 4 + zh], result.at[head, core], near.at[n])

    for n in range(1, NX):
        arrived(part.at[NX + n], part_recv.at[n - 1, 0])
        arrived(stat.at[NX + n], part_recv.at[n - 1, 1])
    slots = [0] + [NX + n for n in range(1, NX)]
    top = stat[0, 0:1, :]
    for n in slots[1:]:
        top = jnp.maximum(top, stat[n, 0:1, :])
    weights = [stat[n, 1:2, :] * jnp.exp2((stat[n, 0:1, :] - top) * SCALE) for n in slots]
    total = weights[0] + weights[1] + weights[2] + weights[3]
    merged = part[0].astype(jnp.float32) * (weights[0] / total)
    for n, w in zip(slots[1:], weights[1:]):
        merged = merged + part[n].astype(jnp.float32) * (w / total)
    ob[...] = ordered(merged.astype(jnp.bfloat16)[:, :SPAN])
    keep(ob, rs, own_b, 0).start()
    deliver(ob, rs, 0, own_b, 0)

    land(qa_h, qa, 5, 5)()
    a_tiles = [(slice(n * TILE, (n + 1) * TILE),) * 2 for n in range(REGION // TILE)]

    def text_rows(ab, kv):
        return txt[:, :, :, ab, kv].reshape(-1, HD)

    def cross(q_tile, keys, values_t):
        s = lax.dot_general(keys, q_tile, NT, preferred_element_type=jnp.float32)
        p = jnp.exp2((s - jnp.max(s, axis=0, keepdims=True)) * SCALE)
        weighted = jnp.dot(values_t, p.astype(jnp.bfloat16), preferred_element_type=jnp.float32)
        return (weighted / jnp.sum(p, axis=0, keepdims=True)).astype(jnp.bfloat16)

    def a_region(i, carry):
        theirs = jnp.logical_or(i == 1, jnp.logical_or(jnp.logical_or(i == 4, i == 5), i == 7))
        cc = jnp.where(theirs, 1 - core, core)
        yy = jnp.where(i < 2, y, jnp.where(i >= 6, yo, jnp.where(lax.rem(i, 2) == 0, ym, yp)))
        n = jnp.where(i < 2, 0, jnp.where(i >= 6, 3, 1 + lax.rem(i, 2)))
        at = cc * NY + yy

        @pl.when(i == 2)
        def _():
            took(a, a_y(ym), 4)
            give(a, a_half(ym, 0), yp, 6)
            share(a, a_y(ym), 1)
            took(a, a_y(yp), 5)
            give(a, a_half(yp, 1), ym, 7)
            share(a, a_y(yp), 2)

        @pl.when(i == 4)
        def _():
            took(a, a_half(yo, 0), 6)
            took(a, a_half(yo, 1), 7)
            share(a, a_y(yo), 3)
            arrived(txt.at[1 - core], text_recv.at[2])
            land(cb_h, cb.at[pl.ds(0, SPAN)], 6, 6)()
            land(ca_h, ca, 7, 7)()
            keys, values_t = text_rows(1, 0), text_rows(1, 1).T
            od[...] = ordered(cross(cb[...], keys, values_t)[:, :SPAN])
            keys, values_t = text_rows(0, 0), text_rows(0, 1).T
            for cols, _ in a_tiles:
                ot[:, cols] = cross(ca[cols, :], keys, values_t)
            for n in range(NX):
                oc[n] = ordered(ot[:, n * SPAN : (n + 1) * SPAN])
            keep(od, rc, own_b, 1).start()
            keep(oc.at[0], rc, own_a, 2).start()
            deliver(od, rc, 0, own_b, 1)
            for n in range(NX):
                deliver(oc.at[n], rc, n, own_a, 1)

        @pl.when(theirs)
        def _():
            for t in range(2):
                arrived(a[t].at[at], twin_recv.at[n, t])

        vt[...] = va[at].T

        def scores(cols, into):
            q_tile = qa[cols, :]
            s = lax.dot_general(ka[at, : REGION - SPAN, :], q_tile, NT, preferred_element_type=jnp.float32)
            into[: REGION - SPAN, :TILE] = s
            e = lax.dot_general(ka[at, REGION - SPAN :, :], q_tile, NT, preferred_element_type=jnp.float32)
            e = e + over(bias_a[pl.ds(pl.multiple_of(at * SPAN, 8), SPAN), :], TILE)
            into[REGION - SPAN :, :TILE] = e
            return jnp.maximum(jnp.max(s, axis=0, keepdims=True), jnp.max(e, axis=0, keepdims=True))

        attend(a_tiles, TILE, scores)
        return carry

    lax.fori_loop(0, NC * NY, a_region, 0)
    for cols, _ in a_tiles:
        ot[:, cols] = (acc[:, cols] / row_l[0:1, cols]).astype(jnp.bfloat16)
    for n in range(NX):
        oa[n] = ordered(ot[:, n * SPAN : (n + 1) * SPAN])
        if n == 0:
            keep(oa.at[0], rs, own_a, 3).start()
        deliver(oa.at[n], rs, n, own_a, 0)

    for s, ref in enumerate((q, c, k, v)):
        arrived(ref.at[pl.ds(0, NX * NZ - 1 + NZ - 1)], send.at[s])
    for t in range(2):
        for n in (0, 1):
            arrived(b_y(y)(b[t]), ring_send.at[n, t])
            arrived(b_half(y, 0)(b[t]), ring_send.at[2 + n, t])
            arrived(a_y(y)(a[t]), ring_send.at[4 + n, t])
            arrived(a_half(y, 0)(a[t]), ring_send.at[6 + n, t])
        for n in range(4):
            arrived(a_y(y)(a[t]), twin_send.at[n, t])
        arrived(b[t].at[core], twin_send.at[4, t])
    for n in range(1, NX):
        arrived(qb.at[n, pl.ds(0, SPAN)], fan_send.at[n - 1])
        arrived(part.at[n], part_send.at[n - 1, 0])
        arrived(stat.at[n], part_send.at[n - 1, 1])
    arrived(txt.at[core, y, pl.ds(0, NX - 1)], text_send.at[0])
    arrived(txt.at[core, pl.ds(0, NY - 1)], text_send.at[1])
    arrived(txt.at[core], text_send.at[2])
    keep(ob, rs, own_b, 0).wait()
    keep(od, rc, own_b, 1).wait()
    keep(oc.at[0], rc, own_a, 2).wait()
    keep(oa.at[0], rs, own_a, 3).wait()
    for n, r in enumerate((rs, rc)):
        moved = r.at[pl.ds(0, (others + NZ * NC - 1) // 2)]
        arrived(moved, out_recv.at[n])
        arrived(moved, out_send.at[n])


def block(q, c, k, v, text, bias_a, bias_b, perm):
    any_spec = pl.BlockSpec(memory_space=pl.ANY)
    vmem = pl.BlockSpec(memory_space=pltpu.VMEM)
    dma = pltpu.SemaphoreType.DMA
    half = lambda *s: pltpu.VMEM(s, jnp.bfloat16)
    full = lambda *s: pltpu.VMEM(s, jnp.float32)
    landing = [REGION, REGION, SPAN, SPAN, REGION, REGION, SPAN, SPAN]
    result = jax.ShapeDtypeStruct((HEADS, NC, PAD, HD), jnp.bfloat16)
    return pl.pallas_call(
        block_kernel,
        in_specs=[any_spec] * 5 + [vmem] * 3,
        out_specs=[any_spec] * 10,
        out_shape=[result] * 2 + [jax.ShapeDtypeStruct((n, HD), jnp.bfloat16) for n in landing],
        scratch_shapes=[
            half(REGION, HD), half(NX, WIDE, HD), half(REGION, HD), half(WIDE, HD),
            half(NC * NY, REGION, HD), half(NC * NY, REGION, HD), half(NC, NY, SPAN, HD), half(NC, NY, SPAN, HD),
            half(NC, NY, NX, 2, 2, 16, HD),
            full(REGION, WIDE), full(REGION, WIDE), half(HD, REGION), full(HD, NX * WIDE),
            full(8, NX * WIDE), full(8, NX * WIDE), half(HD, REGION),
            half(NX, GROUPS, PAD, HD), half(GROUPS, PAD, HD), half(NX, GROUPS, PAD, HD), half(GROUPS, PAD, HD),
            half(2 * NX, HD, WIDE), full(2 * NX, 8, WIDE),
            dma((4,)), dma((8,)), dma((10,)), dma((8, 2)), dma((8, 2)), dma((5, 2)), dma((5, 2)), dma((3,)), dma((3,)),
            dma((3, 2)), dma((3, 2)), dma((3,)), dma((3,)), dma((2,)), dma((2,)), dma((4,)),
        ],
        compiler_params=pltpu.CompilerParams(collective_id=0, has_side_effects=True),
        name="block",
    )(q, c, k, v, text, bias_a, bias_b, perm)[:2]


def order_matrix():
    perm = np.zeros((GROUPS * PAD, NZ * TOK), np.float32)
    for zl in range(2):
        for a in range(2):
            for i in range(TH):
                for zh2 in range(2):
                    for j in range(TW):
                        row = (zl * 8 + a * 4 + i) * PAD + zh2 * TW + j
                        perm[row, (2 * (2 * a + zh2) + zl) * TOK + i * TW + j] = 1
    return jnp.asarray(perm, jnp.bfloat16)


def rope_tables(frame, row, col):
    pair = lax.iota(jnp.int32, HD) // 2
    side = HD // 6
    first = HD // 2 - 2 * side
    in_frames = pair < first
    in_rows = pair < first + side
    numerator = jnp.where(in_frames, pair, jnp.where(in_rows, pair - first, pair - first - side)).astype(jnp.float32)
    denominator = jnp.where(in_frames, first, side).astype(jnp.float32)
    omegas = jnp.power(jnp.float32(10000.0), -(numerator / denominator))
    position = jnp.where(in_frames[None, :], frame[:, None],
                         jnp.where(in_rows[None, :], row[:, None], col[:, None])).astype(jnp.float32)
    angles = position * omegas[None, :]
    sign = jnp.where(lax.iota(jnp.int32, HD) % 2 == 0, -1.0, 1.0)
    return jnp.cos(angles), jnp.sin(angles) * sign[None, :]


def body(self_query, self_key, self_value, cross_query, text_key, text_value, padded_count):
    x, y, z, core = place()
    zl, zh = lax.axis_index("blk_2"), lax.axis_index("uly_0")

    rows = text_key.shape[0]
    text = jnp.stack([text_key, text_value]).reshape(2, rows, LAYER, HD).transpose(2, 0, 1, 3)
    text = lax.ppermute(text, ("blk_2", "uly_1"), [(0, 0), (1, 2), (2, 1), (3, 3)])

    token = lax.iota(jnp.int32, TOK)
    chunk = (x * NY + y) * 2 + zl
    row = lax.rem(chunk, ROW_TILES) * TH + token // TW
    col = (zh * 2 + core) * TW + token % TW
    cos, sin = rope_tables(jnp.full((TOK,), chunk // ROW_TILES), row, col)
    qh, kh, vh, ch = prep(cos, sin, (self_query, self_key, self_value, cross_query))

    order = lax.iota(jnp.int32, LAST)
    n_t, n_z, n_y, n_c = order % TOK, order // TOK % NZ, order // (TOK * NZ) % NY, order // (TOK * NZ * NY)
    n_row = (n_y * 2 + n_z % 2) * TH + n_t // TW
    n_col = (n_z // 2 * 2 + n_c) * TW + n_t % TW
    index = (NX - 1) * GRID_H * GRID_W + n_row * GRID_W + n_col
    bias = jnp.where(index < KEYS - padded_count[0], 0.0, NEG).astype(jnp.float32)
    bias_a = jnp.broadcast_to(bias[:, None], (LAST, HD))
    bias_b = jnp.broadcast_to(jnp.where(x == NX - 1, bias, 0.0)[:, None], (LAST, HD))

    results = block(qh, ch, kh, vh, text, bias_a, bias_b, order_matrix())

    def finish(r):
        r = r[:, :, : 2 * TW].reshape(HEADS, NC, 2, TW, HD)
        return r.transpose(2, 1, 3, 0, 4).reshape(TOK, HEADS * HD)

    return finish(results[0]), finish(results[1])


def solution(mesh):
    split = Mesh(mesh.devices.reshape(4, 4, 2, 4, 2), BLK + ULY)
    own = P(BLK + ULY, None)
    return jax.shard_map(body, mesh=split, in_specs=(own,) * 4 + (P(BLK, ULY),) * 2 + (P(),),
                         out_specs=(own, own), check_vma=False)
```

```python
import functools
import math

import jax
import jax.numpy as jnp
import numpy as np
from jax import lax
from jax.experimental import pallas as pl
from jax.experimental.pallas import tpu as pltpu
from jax.sharding import Mesh
from jax.sharding import PartitionSpec as P

HD = 128
TH = 4
TW = 10
TOK = TH * TW
ROW_TILES = 8
NX, NY, NZ, NC = 4, 4, 8, 2
LAYER = 5
HEADS = NZ * LAYER
GRID_H = TH * ROW_TILES
GRID_W = TW * NZ
KEYS = NX * NY * NZ * NC * TOK
LAST = KEYS // NX
PAD = 24
GROUPS = 16
ULY = ("uly_0", "uly_1")
BLK = ("blk_0", "blk_1", "blk_2")
NEG = -1e30
MESH = pl.DeviceIdType.MESH


def place():
    x = lax.axis_index("blk_0")
    y = lax.axis_index("blk_1")
    z = lax.axis_index("uly_0") * 2 + lax.axis_index("blk_2")
    return x, y, z, lax.axis_index("uly_1")


def at_xz(x, z):
    return {"blk_0": x, "uly_0": z // 2, "blk_2": lax.rem(z, 2)}


SPAN = NZ * TOK
REGION = NX * SPAN
WIDE = 384
TILE = 256
SCALE = math.log2(math.e) / math.sqrt(HD)
NT = (((1,), (1,)), ((), ()))


def block_kernel(
    pad_ref, cos_ref, sin_ref, q_in, k_in, perm, place_in_frame, v, c, text_key, text_value,
    rs, rc, qa_h, ca_h, qb_h, cb_h, ka_h, va_h, kb_h, vb_h,
    q, k, qa, qb, ca, cb, ka, va, kb, vb, txt, s0, s1, vt, vt4, acc, row_m, row_l, ot, oa, ob, oc, od, part, stat,
    send, recv, local, ring_send, ring_recv, twin_send, twin_recv, fan_send, fan_recv, part_send, part_recv,
    text_send, text_recv, out_send, out_recv, near,
):
    x, y, z, core = place()
    zl, zh = lax.axis_index("blk_2"), lax.axis_index("uly_0")
    twin = {"uly_1": 1 - core}
    yp, ym, yo = lax.rem(y + 1, NY), lax.rem(y + NY - 1, NY), lax.rem(y + 2, NY)
    others = NX * NZ * NC - 1

    def owner(n, m):
        ti = lax.rem(zh + m // 4, 4)
        tl = lax.rem(zl + lax.rem(m // 2, 2), 2)
        ta = lax.rem(core + lax.rem(m, 2), 2)
        peer = {"blk_0": lax.rem(x + n, NX), "uly_0": ti, "blk_2": tl, "uly_1": ta}
        return tl * 8 + ta * 4 + ti, peer

    barrier = pltpu.get_barrier_semaphore()

    def greet(n, carry):
        peer = owner(n // GROUPS, lax.rem(n, GROUPS))[1]
        pl.semaphore_signal(barrier, inc=1, device_id=peer, device_id_type=MESH)
        return carry

    lax.fori_loop(1, others + 1, greet, 0)
    for yy in (yp, ym, yo):
        pl.semaphore_signal(barrier, inc=1, device_id={"blk_1": yy}, device_id_type=MESH)

    cos, sin = cos_ref[...], sin_ref[...]
    even = lax.rem(lax.broadcasted_iota(jnp.int32, (TOK, HD), 1), 2) == 0

    def rotate(n, carry):
        for src, dst in ((k_in, k), (q_in, q)):
            for h in range(LAYER):
                wide = src[:, pl.ds(pl.multiple_of((n * LAYER + h) * HD, HD), HD)].astype(jnp.float32)
                partner = jnp.where(even, pltpu.roll(wide, HD - 1, 1), pltpu.roll(wide, 1, 1))
                dst[n * LAYER + h] = (wide * cos + partner * sin).astype(jnp.bfloat16)
        return carry

    lax.fori_loop(0, NZ, rotate, 0)
    pl.semaphore_wait(barrier, others + 3)

    def channels(ref, h):
        return ref.at[:, pl.ds(pl.multiple_of(h * HD, HD), HD)]

    def of_head(ref, h):
        return channels(ref, h) if ref is v or ref is c else ref.at[h]

    def arrived(ref, sem):
        pltpu.make_async_copy(ref, ref, sem).wait()

    def push(src, dst, s, r, peer):
        pltpu.make_async_remote_copy(src, dst, s, r, device_id=peer, device_id_type=MESH).start()

    own_a, own_b = z * LAYER + x, z * LAYER + LAYER - 1

    def rows(ref, start):
        return ref.at[pl.ds(pl.multiple_of(start, 8), TOK)]

    def rows_of(n):
        return n * SPAN + z * TOK

    def send_b(pairs):
        def run(n, carry):
            tz = lax.rem(z + n, NZ)
            h, peer = tz * LAYER + LAYER - 1, at_xz(x, tz)
            for s, src, r, dst in pairs:
                push(of_head(src, h), rows(dst, z * TOK), send.at[s], recv.at[r], peer)
            return carry
        for s, src, r, dst in pairs:
            pltpu.make_async_copy(of_head(src, own_b), rows(dst, z * TOK), recv.at[r]).start()
        lax.fori_loop(1, NZ, run, 0)

    def send_a(pairs, relative):
        def where(tx):
            return rows_of(lax.rem(x - tx + NX, NX)) if relative else rows_of(x)
        def run(n, carry):
            tx, tz = lax.rem(x + n // NZ, NX), lax.rem(z + lax.rem(n, NZ), NZ)
            h, peer = tz * LAYER + tx, at_xz(tx, tz)
            for s, src, r, dst in pairs:
                push(of_head(src, h), rows(dst, where(tx)), send.at[s], recv.at[r], peer)
            return carry
        for s, src, r, dst in pairs:
            pltpu.make_async_copy(of_head(src, own_a), rows(dst, where(x)), recv.at[r]).start()
        lax.fori_loop(1, NX * NZ, run, 0)

    send_b(((2, k, 0, kb_h), (3, v, 1, vb_h), (0, q, 2, qb_h)))
    def text_pieces(n):
        tx = lax.rem(x + n, NX)
        for ab, h in ((0, tx), (1, LAYER - 1)):
            for t, src in enumerate((text_key, text_value)):
                yield channels(src, h), txt.at[zl, y, x, ab, t], {"blk_0": tx, "blk_2": core, "uly_1": zl}

    for n in range(1, NX):
        for src, dst, peer in text_pieces(n):
            push(src, dst, text_send.at[0], text_recv.at[0], peer)

    @pl.when(zl != core)
    def _():
        for src, dst, peer in text_pieces(0):
            push(src, dst, text_send.at[3], text_recv.at[0], peer)

    @pl.when(zl == core)
    def _():
        for src, dst, peer in text_pieces(0):
            pltpu.make_async_copy(src, dst, text_recv.at[0]).start()

    send_a(((2, k, 3, ka_h), (3, v, 4, va_h)), False)
    send_a(((0, q, 5, qa_h),), True)
    send_b(((1, c, 6, cb_h),))
    send_a(((1, c, 7, ca_h),), True)

    qb[:, SPAN:, :] = jnp.zeros((NX, WIDE - SPAN, HD), jnp.bfloat16)
    cb[SPAN:, :] = jnp.zeros((WIDE - SPAN, HD), jnp.bfloat16)
    row_m[...] = jnp.full_like(row_m, NEG)
    row_l[...] = jnp.zeros_like(row_l)
    acc[...] = jnp.zeros_like(acc)
    stat[...] = jnp.zeros_like(stat)

    def give(kind, region, target, n):
        for t, arr in enumerate(kind):
            push(region(arr), region(arr), ring_send.at[n, t], ring_recv.at[n, t], {"blk_1": target})

    def took(kind, region, n):
        for t, arr in enumerate(kind):
            arrived(region(arr), ring_recv.at[n, t])

    def share(kind, region, n):
        for t, arr in enumerate(kind):
            push(region(arr), region(arr), twin_send.at[n, t], twin_recv.at[n, t], twin)

    def land(src, dst, r, n):
        arrived(src, recv.at[r])
        pltpu.make_async_copy(src, dst, local.at[n]).start()
        return lambda: pltpu.make_async_copy(src, dst, local.at[n]).wait()

    a, b = (ka, va), (kb, vb)
    mine = core * NY
    a_y = lambda yy: lambda r: r.at[mine + yy]
    a_half = lambda yy, s: lambda r: r.at[mine + yy, pl.ds(s * (REGION // 2), REGION // 2)]
    b_y = lambda yy: lambda r: r.at[core, yy]
    b_half = lambda yy, s: lambda r: r.at[core, yy, pl.ds(s * (SPAN // 2), SPAN // 2)]
    b_all = lambda r: r.at[core]

    for done in [land(kb_h, kb.at[core, y], 0, 0), land(vb_h, vb.at[core, y], 1, 1)]:
        done()
    give(b, b_y(y), yp, 0)
    give(b, b_y(y), ym, 1)
    land(qb_h, qb.at[0, pl.ds(0, SPAN)], 2, 2)()
    for n in range(1, NX):
        push(qb.at[0, pl.ds(0, SPAN)], qb.at[NX - n, pl.ds(0, SPAN)], fan_send.at[n - 1], fan_recv.at[NX - n - 1],
             {"blk_0": lax.rem(x + n, NX)})
    arrived(txt.at[core, y], text_recv.at[0])
    for yy in (yp, ym, yo):
        push(txt.at[core, y], txt.at[core, y], text_send.at[1], text_recv.at[1], {"blk_1": yy})
    took(b, b_y(ym), 0)
    give(b, b_half(ym, 0), yp, 2)
    took(b, b_y(yp), 1)
    give(b, b_half(yp, 1), ym, 3)
    took(b, b_half(yo, 0), 2)
    took(b, b_half(yo, 1), 3)
    share(b, b_all, 4)
    arrived(txt.at[core, pl.ds(0, NY - 1)], text_recv.at[1])
    push(txt.at[core], txt.at[core], text_send.at[2], text_recv.at[2], twin)
    for n in range(1, NX):
        arrived(qb.at[n, pl.ds(0, SPAN)], fan_recv.at[n - 1])

    held = (s0, s1)

    def absorb(cols, width, s, peak, values):
        m = row_m[0:1, cols]
        new = jnp.maximum(m, peak)
        shrink = jnp.exp2((m - new) * SCALE)
        p = jnp.exp2((s[:, :width] - new) * SCALE)
        row_m[0:1, cols] = new
        row_l[0:1, cols] = row_l[0:1, cols] * shrink + jnp.sum(p, axis=0, keepdims=True)
        acc[:, cols] = acc[:, cols] * shrink + jnp.dot(
            values[...], p.astype(jnp.bfloat16), preferred_element_type=jnp.float32)

    def attend(queries, width, scores):
        peaks = scores(queries[0][0], s0)
        for n, (_, cols) in enumerate(queries):
            ahead = scores(queries[n + 1][0], held[(n + 1) % 2]) if n + 1 < len(queries) else None
            absorb(cols, width, held[n % 2], peaks, vt)
            peaks = ahead

    limit = KEYS - (NX - 1) * LAST - pad_ref[0]
    limit_b = jnp.where(x == NX - 1, limit, LAST)

    def masked(s, cc, yy, bound):
        cells = jnp.concatenate([place_in_frame[...]] * (s.shape[1] // HD), axis=1)
        return jnp.where(cells < bound - yy * (2 * TH * GRID_W) - cc * TW, s, NEG)

    b_tiles = [(n, slice(n * WIDE, (n + 1) * WIDE)) for n in range(NX)]

    def b_region(i, carry):
        cc = lax.rem(core + i, NC)

        @pl.when(i == 1)
        def _():
            for t in range(2):
                arrived(b[t].at[1 - core], twin_recv.at[4, t])

        vt[...] = vb[cc].reshape(REGION, HD).T

        def scores(n, into):
            s = lax.dot_general(kb[cc].reshape(REGION, HD), qb[n], NT, preferred_element_type=jnp.float32)
            peak = jnp.full((1, WIDE), NEG, jnp.float32)
            for yy in range(NY):
                cut = slice(yy * SPAN, (yy + 1) * SPAN)
                e = masked(s[cut], cc, yy, limit_b)
                into[cut, :] = e
                peak = jnp.maximum(peak, jnp.max(e, axis=0, keepdims=True))
            return peak

        attend(b_tiles, WIDE, scores)
        return carry

    lax.fori_loop(0, NC, b_region, 0)
    for n in range(NX):
        cols = slice(n * WIDE, (n + 1) * WIDE)
        part[n] = (acc[:, cols] / row_l[0:1, cols]).astype(jnp.bfloat16)
        stat[n, 0:1, :] = row_m[0:1, cols]
        stat[n, 1:2, :] = row_l[0:1, cols]
    for n in range(1, NX):
        peer = {"blk_0": lax.rem(x + n, NX)}
        push(part.at[n], part.at[NX + n], part_send.at[n - 1, 0], part_recv.at[n - 1, 0], peer)
        push(stat.at[n], stat.at[NX + n], part_send.at[n - 1, 1], part_recv.at[n - 1, 1], peer)

    row_m[...] = jnp.full_like(row_m, NEG)
    row_l[...] = jnp.zeros_like(row_l)
    acc[...] = jnp.zeros_like(acc)

    for done in [land(ka_h, ka.at[mine + y], 3, 3), land(va_h, va.at[mine + y], 4, 4)]:
        done()
    give(a, a_y(y), yp, 4)
    give(a, a_y(y), ym, 5)
    share(a, a_y(y), 0)

    def ordered(cols):
        return lax.dot_general(perm[...], cols, NT, preferred_element_type=jnp.float32).reshape(
            GROUPS, PAD, HD).astype(jnp.bfloat16)

    def deliver(src, result, n, head, which):
        def run(m, carry):
            g, peer = owner(n, m)
            push(src.at[g], result.at[head, core], out_send.at[which], out_recv.at[which], peer)
            return carry
        lax.fori_loop(1 if n == 0 else 0, GROUPS, run, 0)

    def keep(src, result, head, n):
        return pltpu.make_async_copy(src.at[zl * 8 + core * 4 + zh], result.at[head, core], near.at[n])

    for n in range(1, NX):
        arrived(part.at[NX + n], part_recv.at[n - 1, 0])
        arrived(stat.at[NX + n], part_recv.at[n - 1, 1])
    slots = [0] + [NX + n for n in range(1, NX)]
    top = stat[0, 0:1, :]
    for n in slots[1:]:
        top = jnp.maximum(top, stat[n, 0:1, :])
    weights = [stat[n, 1:2, :] * jnp.exp2((stat[n, 0:1, :] - top) * SCALE) for n in slots]
    total = weights[0] + weights[1] + weights[2] + weights[3]
    merged = part[0].astype(jnp.float32) * (weights[0] / total)
    for n, w in zip(slots[1:], weights[1:]):
        merged = merged + part[n].astype(jnp.float32) * (w / total)
    ob[...] = ordered(merged.astype(jnp.bfloat16)[:, :SPAN])
    keep(ob, rs, own_b, 0).start()
    deliver(ob, rs, 0, own_b, 0)

    land(qa_h, qa, 5, 5)()
    a_tiles = [(slice(n * TILE, (n + 1) * TILE),) * 2 for n in range(REGION // TILE)]

    def text_rows(ab, kv):
        return txt[:, :, :, ab, kv].reshape(-1, HD)

    def cross(q_tile, keys, values_t):
        s = lax.dot_general(keys, q_tile, NT, preferred_element_type=jnp.float32)
        p = jnp.exp2((s - jnp.max(s, axis=0, keepdims=True)) * SCALE)
        weighted = jnp.dot(values_t, p.astype(jnp.bfloat16), preferred_element_type=jnp.float32)
        return (weighted / jnp.sum(p, axis=0, keepdims=True)).astype(jnp.bfloat16)

    def region_of(i):
        theirs = jnp.logical_or(i == 1, jnp.logical_or(jnp.logical_or(i == 4, i == 5), i == 7))
        cc = jnp.where(theirs, 1 - core, core)
        yy = jnp.where(i < 2, y, jnp.where(i >= 6, yo, jnp.where(lax.rem(i, 2) == 0, ym, yp)))
        return cc, yy, cc * NY + yy

    def a_scores(region, cols, into):
        cc, yy, at = region
        q_tile = qa[cols, :]
        s = lax.dot_general(ka[at, : REGION - SPAN, :], q_tile, NT, preferred_element_type=jnp.float32)
        into[: REGION - SPAN, :TILE] = s
        e = lax.dot_general(ka[at, REGION - SPAN :, :], q_tile, NT, preferred_element_type=jnp.float32)
        e = masked(e, cc, yy, limit)
        into[REGION - SPAN :, :TILE] = e
        return jnp.maximum(jnp.max(s, axis=0, keepdims=True), jnp.max(e, axis=0, keepdims=True))

    def a_region(i, carry):
        region = region_of(i)

        @pl.when(i == 1)
        def _():
            for t in range(2):
                arrived(a[t].at[region[2]], twin_recv.at[0, t])

        @pl.when(i == 2)
        def _():
            took(a, a_y(ym), 4)
            give(a, a_half(ym, 0), yp, 6)
            share(a, a_y(ym), 1)
            took(a, a_y(yp), 5)
            give(a, a_half(yp, 1), ym, 7)
            share(a, a_y(yp), 2)

        vt[...] = va[region[2]].T
        attend(a_tiles, TILE, lambda cols, into: a_scores(region, cols, into))
        return carry

    lax.fori_loop(0, 4, a_region, 0)
    took(a, a_half(yo, 0), 6)
    took(a, a_half(yo, 1), 7)
    share(a, a_y(yo), 3)

    arrived(txt.at[1 - core], text_recv.at[2])
    land(cb_h, cb.at[pl.ds(0, SPAN)], 6, 6)()
    land(ca_h, ca, 7, 7)()
    keys, values_t = text_rows(1, 0), text_rows(1, 1).T
    od[...] = ordered(cross(cb[...], keys, values_t)[:, :SPAN])
    keep(od, rc, own_b, 1).start()
    deliver(od, rc, 0, own_b, 1)
    keys, values_t = text_rows(0, 0), text_rows(0, 1).T
    for cols, _ in a_tiles:
        ot[:, cols] = cross(ca[cols, :], keys, values_t)
    for n in range(NX):
        oc[n] = ordered(ot[:, n * SPAN : (n + 1) * SPAN])
    keep(oc.at[0], rc, own_a, 2).start()
    for n in range(NX):
        deliver(oc.at[n], rc, n, own_a, 1)

    last = [region_of(i) for i in (4, 5, 6, 7)]
    for (cc, yy, at), n in ((last[0], 1), (last[1], 2), (last[3], 3)):
        for t in range(2):
            arrived(a[t].at[at], twin_recv.at[n, t])
    for n, region in enumerate(last):
        vt4[n] = va[region[2]].T

    def a_tile(t, peak):
        cols = pl.ds(pl.multiple_of(t * TILE, TILE), TILE)
        after = pl.ds(pl.multiple_of(jnp.minimum(t + 1, REGION // TILE - 1) * TILE, TILE), TILE)
        for n in range(4):
            if n < 3:
                ahead = a_scores(last[n + 1], cols, held[(n + 1) % 2])
            else:
                ahead = a_scores(last[0], after, held[0])
            absorb(cols, TILE, held[n % 2], peak, vt4.at[n])
            peak = ahead
        ot[:, cols] = (acc[:, cols] / row_l[0:1, cols]).astype(jnp.bfloat16)
        for n in range(NX):
            @pl.when(t == n + 1)
            def _():
                oa[n] = ordered(ot[:, n * SPAN : (n + 1) * SPAN])
                if n == 0:
                    keep(oa.at[0], rs, own_a, 3).start()
                deliver(oa.at[n], rs, n, own_a, 0)
        return peak

    lax.fori_loop(0, REGION // TILE, a_tile, a_scores(last[0], slice(0, TILE), held[0]))

    for n in range(4):
        arrived(v.at[:, pl.ds(0, (NX * NZ - 1 + NZ - 1) * HD)], send.at[n])
    for t in range(2):
        for n in (0, 1):
            arrived(b_y(y)(b[t]), ring_send.at[n, t])
            arrived(b_half(y, 0)(b[t]), ring_send.at[2 + n, t])
            arrived(a_y(y)(a[t]), ring_send.at[4 + n, t])
            arrived(a_half(y, 0)(a[t]), ring_send.at[6 + n, t])
        for n in range(4):
            arrived(a_y(y)(a[t]), twin_send.at[n, t])
        arrived(b[t].at[core], twin_send.at[4, t])
    for n in range(1, NX):
        arrived(qb.at[n, pl.ds(0, SPAN)], fan_send.at[n - 1])
        arrived(part.at[n], part_send.at[n - 1, 0])
        arrived(stat.at[n], part_send.at[n - 1, 1])
    arrived(txt.at[core, y, pl.ds(0, NX - 1)], text_send.at[0])

    @pl.when(zl != core)
    def _():
        arrived(txt.at[core, y, 0], text_send.at[3])

    arrived(txt.at[core, pl.ds(0, NY - 1)], text_send.at[1])
    arrived(txt.at[core], text_send.at[2])
    keep(ob, rs, own_b, 0).wait()
    keep(od, rc, own_b, 1).wait()
    keep(oc.at[0], rc, own_a, 2).wait()
    keep(oa.at[0], rs, own_a, 3).wait()
    for n, r in enumerate((rs, rc)):
        moved = r.at[pl.ds(0, (others + NZ * NC - 1) // 2)]
        arrived(moved, out_recv.at[n])
        arrived(moved, out_send.at[n])


def block(pad, cos, sin, q, k, v, c, text_key, text_value, perm, cells):
    any_spec = pl.BlockSpec(memory_space=pl.ANY)
    vmem = pl.BlockSpec(memory_space=pltpu.VMEM)
    dma = pltpu.SemaphoreType.DMA
    half = lambda *s: pltpu.VMEM(s, jnp.bfloat16)
    full = lambda *s: pltpu.VMEM(s, jnp.float32)
    landing = [REGION, REGION, SPAN, SPAN, REGION, REGION, SPAN, SPAN]
    result = jax.ShapeDtypeStruct((HEADS, NC, PAD, HD), jnp.bfloat16)
    return pl.pallas_call(
        block_kernel,
        in_specs=[pl.BlockSpec(memory_space=pltpu.SMEM)] + [vmem] * 6 + [any_spec] * 4,
        out_specs=[any_spec] * 10,
        out_shape=[result] * 2 + [jax.ShapeDtypeStruct((n, HD), jnp.bfloat16) for n in landing],
        scratch_shapes=[
            half(HEADS, TOK, HD), half(HEADS, TOK, HD),
            half(REGION, HD), half(NX, WIDE, HD), half(REGION, HD), half(WIDE, HD),
            half(NC * NY, REGION, HD), half(NC * NY, REGION, HD), half(NC, NY, SPAN, HD), half(NC, NY, SPAN, HD),
            half(NC, NY, NX, 2, 2, 16, HD),
            full(REGION, WIDE), full(REGION, WIDE), half(HD, REGION), half(4, HD, REGION), full(HD, NX * WIDE),
            full(8, NX * WIDE), full(8, NX * WIDE), half(HD, REGION),
            half(NX, GROUPS, PAD, HD), half(GROUPS, PAD, HD), half(NX, GROUPS, PAD, HD), half(GROUPS, PAD, HD),
            half(2 * NX, HD, WIDE), full(2 * NX, 8, WIDE),
            dma((4,)), dma((8,)), dma((10,)), dma((8, 2)), dma((8, 2)), dma((5, 2)), dma((5, 2)), dma((3,)), dma((3,)),
            dma((3, 2)), dma((3, 2)), dma((4,)), dma((3,)), dma((2,)), dma((2,)), dma((4,)),
        ],
        compiler_params=pltpu.CompilerParams(collective_id=0, has_side_effects=True),
        name="block",
    )(pad, cos, sin, q, k, perm, cells, v, c, text_key, text_value)[:2]


def frame_cells():
    z, i, j = np.meshgrid(np.arange(NZ), np.arange(TH), np.arange(TW), indexing="ij")
    cells = (z % 2) * TH * GRID_W + i * GRID_W + (z // 2) * 2 * TW + j
    return jnp.asarray(np.broadcast_to(cells.reshape(-1, 1), (SPAN, HD)), jnp.int32)


def order_matrix():
    perm = np.zeros((GROUPS * PAD, NZ * TOK), np.float32)
    for zl in range(2):
        for a in range(2):
            for i in range(TH):
                for zh2 in range(2):
                    for j in range(TW):
                        row = (zl * 8 + a * 4 + i) * PAD + zh2 * TW + j
                        perm[row, (2 * (2 * a + zh2) + zl) * TOK + i * TW + j] = 1
    return jnp.asarray(perm, jnp.bfloat16)


def rope_tables(frame, row, col):
    pair = lax.iota(jnp.int32, HD) // 2
    side = HD // 6
    first = HD // 2 - 2 * side
    in_frames = pair < first
    in_rows = pair < first + side
    numerator = jnp.where(in_frames, pair, jnp.where(in_rows, pair - first, pair - first - side)).astype(jnp.float32)
    denominator = jnp.where(in_frames, first, side).astype(jnp.float32)
    omegas = jnp.power(jnp.float32(10000.0), -(numerator / denominator))
    position = jnp.where(in_frames[None, :], frame[:, None],
                         jnp.where(in_rows[None, :], row[:, None], col[:, None])).astype(jnp.float32)
    angles = position * omegas[None, :]
    sign = jnp.where(lax.iota(jnp.int32, HD) % 2 == 0, -1.0, 1.0)
    return jnp.cos(angles), jnp.sin(angles) * sign[None, :]


def body(self_query, self_key, self_value, cross_query, text_key, text_value, padded_count):
    x, y, z, core = place()
    zl, zh = lax.axis_index("blk_2"), lax.axis_index("uly_0")

    token = lax.iota(jnp.int32, TOK)
    chunk = (x * NY + y) * 2 + zl
    row = lax.rem(chunk, ROW_TILES) * TH + token // TW
    col = (zh * 2 + core) * TW + token % TW
    cos, sin = rope_tables(jnp.full((TOK,), chunk // ROW_TILES), row, col)
    results = block(padded_count, cos, sin, self_query, self_key, self_value, cross_query, text_key, text_value,
                    order_matrix(), frame_cells())

    def finish(r):
        r = r[:, :, : 2 * TW].reshape(HEADS, NC, 2, TW, HD)
        return r.transpose(2, 1, 3, 0, 4).reshape(TOK, HEADS * HD)

    return finish(results[0]), finish(results[1])


def solution(mesh):
    split = Mesh(mesh.devices.reshape(4, 4, 2, 4, 2), BLK + ULY)
    own = P(BLK + ULY, None)
    return jax.shard_map(body, mesh=split, in_specs=(own,) * 4 + (P(BLK, ULY),) * 2 + (P(),),
                         out_specs=(own, own), check_vma=False)
```

```python
import functools
import math

import jax
import jax.numpy as jnp
import numpy as np
from jax import lax
from jax.experimental import pallas as pl
from jax.experimental.pallas import tpu as pltpu
from jax.sharding import Mesh
from jax.sharding import PartitionSpec as P

HD = 128
TH = 4
TW = 10
TOK = TH * TW
ROW_TILES = 8
NX, NY, NZ, NC = 4, 4, 8, 2
LAYER = 5
HEADS = NZ * LAYER
GRID_H = TH * ROW_TILES
GRID_W = TW * NZ
KEYS = NX * NY * NZ * NC * TOK
LAST = KEYS // NX
PAD = 24
GROUPS = 16
ULY = ("uly_0", "uly_1")
BLK = ("blk_0", "blk_1", "blk_2")
NEG = -1e30
MESH = pl.DeviceIdType.MESH


def place():
    x = lax.axis_index("blk_0")
    y = lax.axis_index("blk_1")
    z = lax.axis_index("uly_0") * 2 + lax.axis_index("blk_2")
    return x, y, z, lax.axis_index("uly_1")


def at_xz(x, z):
    return {"blk_0": x, "uly_0": z // 2, "blk_2": lax.rem(z, 2)}


SPAN = NZ * TOK
REGION = NX * SPAN
WIDE = 384
TILE = 256
SCALE = math.log2(math.e) / math.sqrt(HD)
NT = (((1,), (1,)), ((), ()))


def block_kernel(
    pad_ref, omegas, perm, place_in_frame, q_hbm, k_hbm, v, c, text_key, text_value,
    rs, rc, qa_h, ca_h, qb_h, cb_h, ka_h, va_h, kb_h, vb_h,
    q_in, k_in, q, k, qa, qb, ca, cb, ka, va, kb, vb, txt, s0, s1, vt, vt4, acc, row_m, row_l, ot, oa, ob, oc, od, part, stat,
    send, recv, local, ring_send, ring_recv, twin_send, twin_recv, fan_send, fan_recv, part_send, part_recv,
    text_send, text_recv, out_send, out_recv, near,
):
    x, y, z, core = place()
    zl, zh = lax.axis_index("blk_2"), lax.axis_index("uly_0")
    twin = {"uly_1": 1 - core}
    yp, ym, yo = lax.rem(y + 1, NY), lax.rem(y + NY - 1, NY), lax.rem(y + 2, NY)
    others = NX * NZ * NC - 1

    def owner(n, m):
        ti = lax.rem(zh + m // 4, 4)
        tl = lax.rem(zl + lax.rem(m // 2, 2), 2)
        ta = lax.rem(core + lax.rem(m, 2), 2)
        peer = {"blk_0": lax.rem(x + n, NX), "uly_0": ti, "blk_2": tl, "uly_1": ta}
        return tl * 8 + ta * 4 + ti, peer

    loads = [pltpu.make_async_copy(k_hbm, k_in, local.at[8]), pltpu.make_async_copy(q_hbm, q_in, local.at[9])]
    for load in loads:
        load.start()
    barrier = pltpu.get_barrier_semaphore()

    def greet(n, carry):
        rest = lax.rem(n, GROUPS)
        peer = owner(lax.rem(6 - n // GROUPS, 4), lax.rem(6 - rest // 4, 4) * 4 + lax.rem(rest, 4))[1]
        pl.semaphore_signal(barrier, inc=1, device_id=peer, device_id_type=MESH)
        return carry

    home = 2 * GROUPS + 2 * 4
    lax.fori_loop(0, home, greet, 0)
    lax.fori_loop(home + 1, others + 1, greet, 0)
    for yy in (yp, ym, yo):
        pl.semaphore_signal(barrier, inc=1, device_id={"blk_1": yy}, device_id_type=MESH)

    token = lax.broadcasted_iota(jnp.int32, (TOK, HD), 0)
    chunk = (x * NY + y) * 2 + zl
    row = lax.rem(chunk, ROW_TILES) * TH + token // TW
    col = (zh * 2 + core) * TW + lax.rem(token, TW)
    angles = (jnp.full((TOK, HD), chunk // ROW_TILES).astype(jnp.float32) * omegas[0:1, :]
              + row.astype(jnp.float32) * omegas[1:2, :] + col.astype(jnp.float32) * omegas[2:3, :])
    cos, sin = jnp.cos(angles), jnp.sin(angles) * omegas[3:4, :]
    for load in loads:
        load.wait()
    even = lax.rem(lax.broadcasted_iota(jnp.int32, (TOK, HD), 1), 2) == 0

    def rotate(n, carry):
        for src, dst in ((k_in, k), (q_in, q)):
            for h in range(LAYER):
                wide = src[:, pl.ds(pl.multiple_of((n * LAYER + h) * HD, HD), HD)].astype(jnp.float32)
                partner = jnp.where(even, pltpu.roll(wide, HD - 1, 1), pltpu.roll(wide, 1, 1))
                dst[n * LAYER + h] = (wide * cos + partner * sin).astype(jnp.bfloat16)
        return carry

    lax.fori_loop(0, NZ, rotate, 0)
    pl.semaphore_wait(barrier, others + 3)

    def channels(ref, h):
        return ref.at[:, pl.ds(pl.multiple_of(h * HD, HD), HD)]

    def of_head(ref, h):
        return channels(ref, h) if ref is v or ref is c else ref.at[h]

    def arrived(ref, sem):
        pltpu.make_async_copy(ref, ref, sem).wait()

    def push(src, dst, s, r, peer):
        pltpu.make_async_remote_copy(src, dst, s, r, device_id=peer, device_id_type=MESH).start()

    own_a, own_b = z * LAYER + x, z * LAYER + LAYER - 1

    def rows(ref, start):
        return ref.at[pl.ds(pl.multiple_of(start, 8), TOK)]

    def rows_of(n):
        return n * SPAN + z * TOK

    def send_b(pairs):
        def run(n, carry):
            tz = lax.rem(z + n, NZ)
            h, peer = tz * LAYER + LAYER - 1, at_xz(x, tz)
            for s, src, r, dst in pairs:
                push(of_head(src, h), rows(dst, z * TOK), send.at[s], recv.at[r], peer)
            return carry
        for s, src, r, dst in pairs:
            pltpu.make_async_copy(of_head(src, own_b), rows(dst, z * TOK), recv.at[r]).start()
        lax.fori_loop(1, NZ, run, 0)

    def send_a(pairs, relative):
        def where(tx):
            return rows_of(lax.rem(x - tx + NX + NX - 1, NX)) if relative else rows_of(x)
        def run(n, carry):
            tx, tz = lax.rem(x + n // NZ, NX), lax.rem(z + lax.rem(n, NZ), NZ)
            h, peer = tz * LAYER + tx, at_xz(tx, tz)
            for s, src, r, dst in pairs:
                push(of_head(src, h), rows(dst, where(tx)), send.at[s], recv.at[r], peer)
            return carry
        for s, src, r, dst in pairs:
            pltpu.make_async_copy(of_head(src, own_a), rows(dst, where(x)), recv.at[r]).start()
        lax.fori_loop(1, NX * NZ, run, 0)

    send_b(((2, k, 0, kb_h), (3, v, 1, vb_h), (0, q, 2, qb_h)))
    def text_pieces(n):
        tx = lax.rem(x + n, NX)
        for ab, h in ((0, tx), (1, LAYER - 1)):
            for t, src in enumerate((text_key, text_value)):
                yield channels(src, h), txt.at[zl, y, x, ab, t], {"blk_0": tx, "blk_2": core, "uly_1": zl}

    for n in range(1, NX):
        for src, dst, peer in text_pieces(n):
            push(src, dst, text_send.at[0], text_recv.at[0], peer)

    @pl.when(zl != core)
    def _():
        for src, dst, peer in text_pieces(0):
            push(src, dst, text_send.at[3], text_recv.at[0], peer)

    @pl.when(zl == core)
    def _():
        for src, dst, peer in text_pieces(0):
            pltpu.make_async_copy(src, dst, text_recv.at[0]).start()

    send_a(((2, k, 3, ka_h),), False)
    send_a(((3, v, 4, va_h),), False)
    send_b(((1, c, 6, cb_h),))
    send_a(((1, c, 7, ca_h),), True)
    send_a(((0, q, 5, qa_h),), True)

    qb[:, SPAN:, :] = jnp.zeros((NX, WIDE - SPAN, HD), jnp.bfloat16)
    cb[SPAN:, :] = jnp.zeros((WIDE - SPAN, HD), jnp.bfloat16)
    row_m[...] = jnp.full_like(row_m, NEG)
    row_l[...] = jnp.zeros_like(row_l)
    acc[...] = jnp.zeros_like(acc)
    stat[...] = jnp.zeros_like(stat)

    def give(kind, region, target, n, which=(0, 1)):
        for t in which:
            push(region(kind[t]), region(kind[t]), ring_send.at[n, t], ring_recv.at[n, t], {"blk_1": target})

    def took(kind, region, n, which=(0, 1)):
        for t in which:
            arrived(region(kind[t]), ring_recv.at[n, t])

    def share(kind, region, n, which=(0, 1)):
        for t in which:
            push(region(kind[t]), region(kind[t]), twin_send.at[n, t], twin_recv.at[n, t], twin)

    def land(src, dst, r, n):
        arrived(src, recv.at[r])
        pltpu.make_async_copy(src, dst, local.at[n]).start()
        return lambda: pltpu.make_async_copy(src, dst, local.at[n]).wait()

    a, b = (ka, va), (kb, vb)
    mine = core * NY
    a_y = lambda yy: lambda r: r.at[mine + yy]
    a_half = lambda yy, s: lambda r: r.at[mine + yy, pl.ds(s * (REGION // 2), REGION // 2)]
    b_y = lambda yy: lambda r: r.at[core, yy]
    b_half = lambda yy, s: lambda r: r.at[core, yy, pl.ds(s * (SPAN // 2), SPAN // 2)]
    b_all = lambda r: r.at[core]

    for done in [land(kb_h, kb.at[core, y], 0, 0), land(vb_h, vb.at[core, y], 1, 1)]:
        done()
    give(b, b_y(y), yp, 0)
    give(b, b_y(y), ym, 1)
    land(qb_h, qb.at[0, pl.ds(0, SPAN)], 2, 2)()
    for n in range(1, NX):
        push(qb.at[0, pl.ds(0, SPAN)], qb.at[NX - n, pl.ds(0, SPAN)], fan_send.at[n - 1], fan_recv.at[NX - n - 1],
             {"blk_0": lax.rem(x + n, NX)})
    arrived(txt.at[core, y], text_recv.at[0])
    for yy in (yp, ym, yo):
        push(txt.at[core, y], txt.at[core, y], text_send.at[1], text_recv.at[1], {"blk_1": yy})
    took(b, b_y(ym), 0)
    give(b, b_half(ym, 0), yp, 2)
    took(b, b_y(yp), 1)
    give(b, b_half(yp, 1), ym, 3)
    took(b, b_half(yo, 0), 2)
    took(b, b_half(yo, 1), 3)
    share(b, b_all, 4)
    arrived(txt.at[core, pl.ds(0, NY - 1)], text_recv.at[1])
    push(txt.at[core], txt.at[core], text_send.at[2], text_recv.at[2], twin)
    for n in range(1, NX):
        arrived(qb.at[n, pl.ds(0, SPAN)], fan_recv.at[n - 1])

    held = (s0, s1)

    def absorb(cols, width, s, peak, values):
        m = row_m[0:1, cols]
        new = jnp.maximum(m, peak)
        shrink = jnp.exp2((m - new) * SCALE)
        p = jnp.exp2((s[:, :width] - new) * SCALE)
        row_m[0:1, cols] = new
        row_l[0:1, cols] = row_l[0:1, cols] * shrink + jnp.sum(p, axis=0, keepdims=True)
        acc[:, cols] = acc[:, cols] * shrink + jnp.dot(
            values[...], p.astype(jnp.bfloat16), preferred_element_type=jnp.float32)

    def attend(queries, width, scores):
        peaks = scores(queries[0][0], s0)
        for n, (_, cols) in enumerate(queries):
            ahead = scores(queries[n + 1][0], held[(n + 1) % 2]) if n + 1 < len(queries) else None
            absorb(cols, width, held[n % 2], peaks, vt)
            peaks = ahead

    limit = KEYS - (NX - 1) * LAST - pad_ref[0]
    limit_b = jnp.where(x == NX - 1, limit, LAST)

    def masked(s, cc, yy, bound):
        cells = jnp.concatenate([place_in_frame[...]] * (s.shape[1] // HD), axis=1)
        return jnp.where(cells < bound - yy * (2 * TH * GRID_W) - cc * TW, s, NEG)

    def own_region(t):
        land((ka_h, va_h)[t], a[t].at[mine + y], 3 + t, 3 + t)()
        give(a, a_y(y), yp, 4, (t,))
        give(a, a_y(y), ym, 5, (t,))
        share(a, a_y(y), 0, (t,))

    def pass_on(t):
        took(a, a_y(ym), 4, (t,))
        give(a, a_half(ym, 0), yp, 6, (t,))
        share(a, a_y(ym), 1, (t,))
        took(a, a_y(yp), 5, (t,))
        give(a, a_half(yp, 1), ym, 7, (t,))
        share(a, a_y(yp), 2, (t,))

    b_tiles = [(n, slice(n * WIDE, (n + 1) * WIDE)) for n in range(NX)]

    def b_region(i, carry):
        cc = lax.rem(core + i, NC)

        @pl.when(i == 1)
        def _():
            for t in range(2):
                arrived(b[t].at[1 - core], twin_recv.at[4, t])

        vt[...] = vb[cc].reshape(REGION, HD).T

        def scores(n, into):
            s = lax.dot_general(kb[cc].reshape(REGION, HD), qb[n], NT, preferred_element_type=jnp.float32)
            peak = jnp.full((1, WIDE), NEG, jnp.float32)
            for yy in range(NY):
                cut = slice(yy * SPAN, (yy + 1) * SPAN)
                e = masked(s[cut], cc, yy, limit_b)
                into[cut, :] = e
                peak = jnp.maximum(peak, jnp.max(e, axis=0, keepdims=True))
            return peak

        attend(b_tiles, WIDE, scores)
        return carry

    own_region(0)
    lax.fori_loop(0, NC, b_region, 0)
    for n in range(NX):
        cols = slice(n * WIDE, (n + 1) * WIDE)
        part[n] = (acc[:, cols] / row_l[0:1, cols]).astype(jnp.bfloat16)
        stat[n, 0:1, :] = row_m[0:1, cols]
        stat[n, 1:2, :] = row_l[0:1, cols]
    for n in range(1, NX):
        peer = {"blk_0": lax.rem(x + n, NX)}
        push(part.at[n], part.at[NX + n], part_send.at[n - 1, 0], part_recv.at[n - 1, 0], peer)
        push(stat.at[n], stat.at[NX + n], part_send.at[n - 1, 1], part_recv.at[n - 1, 1], peer)

    row_m[...] = jnp.full_like(row_m, NEG)
    row_l[...] = jnp.zeros_like(row_l)
    acc[...] = jnp.zeros_like(acc)

    own_region(1)
    pass_on(0)

    def ordered(cols):
        return lax.dot_general(perm[...], cols, NT, preferred_element_type=jnp.float32).reshape(
            GROUPS, PAD, HD).astype(jnp.bfloat16)

    def deliver(src, result, n, head, which):
        def run(m, carry):
            g, peer = owner(n, m)
            push(src.at[g], result.at[head, core], out_send.at[which], out_recv.at[which], peer)
            return carry
        lax.fori_loop(1 if n == 0 else 0, GROUPS, run, 0)

    def keep(src, result, head, n):
        return pltpu.make_async_copy(src.at[zl * 8 + core * 4 + zh], result.at[head, core], near.at[n])

    a_tiles = [(slice(n * TILE, (n + 1) * TILE),) * 2 for n in range(REGION // TILE)]

    def text_rows(ab, kv):
        return txt[:, :, :, ab, kv].reshape(-1, HD)

    def cross(q_tile, keys, values_t):
        s = lax.dot_general(keys, q_tile, NT, preferred_element_type=jnp.float32)
        p = jnp.exp2((s - jnp.max(s, axis=0, keepdims=True)) * SCALE)
        weighted = jnp.dot(values_t, p.astype(jnp.bfloat16), preferred_element_type=jnp.float32)
        return (weighted / jnp.sum(p, axis=0, keepdims=True)).astype(jnp.bfloat16)

    def merge_parts():
        for n in range(1, NX):
            arrived(part.at[NX + n], part_recv.at[n - 1, 0])
            arrived(stat.at[NX + n], part_recv.at[n - 1, 1])
        slots = [0] + [NX + n for n in range(1, NX)]
        top = stat[0, 0:1, :]
        for n in slots[1:]:
            top = jnp.maximum(top, stat[n, 0:1, :])
        weights = [stat[n, 1:2, :] * jnp.exp2((stat[n, 0:1, :] - top) * SCALE) for n in slots]
        total = weights[0] + weights[1] + weights[2] + weights[3]
        merged = part[0].astype(jnp.float32) * (weights[0] / total)
        for n, w in zip(slots[1:], weights[1:]):
            merged = merged + part[n].astype(jnp.float32) * (w / total)
        ob[...] = ordered(merged.astype(jnp.bfloat16)[:, :SPAN])
        keep(ob, rs, own_b, 0).start()
        deliver(ob, rs, 0, own_b, 0)

    def attend_text():
        arrived(txt.at[1 - core], text_recv.at[2])
        land(cb_h, cb.at[pl.ds(0, SPAN)], 6, 6)()
        land(ca_h, ca, 7, 7)()
        keys, values_t = text_rows(1, 0), text_rows(1, 1).T
        od[...] = ordered(cross(cb[...], keys, values_t)[:, :SPAN])
        keep(od, rc, own_b, 1).start()
        deliver(od, rc, 0, own_b, 1)
        keys, values_t = text_rows(0, 0), text_rows(0, 1).T
        for cols, _ in a_tiles:
            ot[:, cols] = cross(ca[cols, :], keys, values_t)
        for n in range(NX):
            oc[n] = ordered(ot[:, n * SPAN : (n + 1) * SPAN])
        keep(oc.at[NX - 1], rc, own_a, 2).start()
        for n in range(NX):
            deliver(oc.at[n], rc, (n + 1) % NX, own_a, 1)

    def region_of(i):
        theirs = jnp.logical_or(i == 1, jnp.logical_or(jnp.logical_or(i == 4, i == 5), i == 7))
        cc = jnp.where(theirs, 1 - core, core)
        yy = jnp.where(i < 2, y, jnp.where(i >= 6, yo, jnp.where(lax.rem(i, 2) == 0, ym, yp)))
        return cc, yy, cc * NY + yy

    def a_scores(region, cols, into):
        cc, yy, at = region
        q_tile = qa[cols, :]
        s = lax.dot_general(ka[at, : REGION - SPAN, :], q_tile, NT, preferred_element_type=jnp.float32)
        into[: REGION - SPAN, :TILE] = s
        e = lax.dot_general(ka[at, REGION - SPAN :, :], q_tile, NT, preferred_element_type=jnp.float32)
        e = masked(e, cc, yy, limit)
        into[REGION - SPAN :, :TILE] = e
        return jnp.maximum(jnp.max(s, axis=0, keepdims=True), jnp.max(e, axis=0, keepdims=True))

    def a_region(i, carry):
        region = region_of(i)

        @pl.when(i == 1)
        def _():
            for t in range(2):
                arrived(a[t].at[region[2]], twin_recv.at[0, t])

        vt[...] = va[region[2]].T
        attend(a_tiles, TILE, lambda cols, into: a_scores(region, cols, into))
        return carry

    attend_text()
    pass_on(1)
    merge_parts()
    land(qa_h, qa, 5, 5)()
    lax.fori_loop(0, 4, a_region, 0)
    took(a, a_half(yo, 0), 6)
    took(a, a_half(yo, 1), 7)
    share(a, a_y(yo), 3)

    last = [region_of(i) for i in (4, 5, 6, 7)]
    for (cc, yy, at), n in ((last[0], 1), (last[1], 2), (last[3], 3)):
        for t in range(2):
            arrived(a[t].at[at], twin_recv.at[n, t])
    for n, region in enumerate(last):
        vt4[n] = va[region[2]].T

    def a_tile(t, peak):
        cols = pl.ds(pl.multiple_of(t * TILE, TILE), TILE)
        after = pl.ds(pl.multiple_of(jnp.minimum(t + 1, REGION // TILE - 1) * TILE, TILE), TILE)
        for n in range(4):
            if n < 3:
                ahead = a_scores(last[n + 1], cols, held[(n + 1) % 2])
            else:
                ahead = a_scores(last[0], after, held[0])
            absorb(cols, TILE, held[n % 2], peak, vt4.at[n])
            peak = ahead
        ot[:, cols] = (acc[:, cols] / row_l[0:1, cols]).astype(jnp.bfloat16)
        for n in range(NX):
            @pl.when(t == n + 1)
            def _():
                oa[n] = ordered(ot[:, n * SPAN : (n + 1) * SPAN])
                if n == NX - 1:
                    keep(oa.at[n], rs, own_a, 3).start()
                deliver(oa.at[n], rs, (n + 1) % NX, own_a, 0)
        return peak

    lax.fori_loop(0, REGION // TILE, a_tile, a_scores(last[0], slice(0, TILE), held[0]))

    for n in range(4):
        arrived(v.at[:, pl.ds(0, (NX * NZ - 1 + NZ - 1) * HD)], send.at[n])
    for t in range(2):
        for n in (0, 1):
            arrived(b_y(y)(b[t]), ring_send.at[n, t])
            arrived(b_half(y, 0)(b[t]), ring_send.at[2 + n, t])
            arrived(a_y(y)(a[t]), ring_send.at[4 + n, t])
            arrived(a_half(y, 0)(a[t]), ring_send.at[6 + n, t])
        for n in range(4):
            arrived(a_y(y)(a[t]), twin_send.at[n, t])
        arrived(b[t].at[core], twin_send.at[4, t])
    for n in range(1, NX):
        arrived(qb.at[n, pl.ds(0, SPAN)], fan_send.at[n - 1])
        arrived(part.at[n], part_send.at[n - 1, 0])
        arrived(stat.at[n], part_send.at[n - 1, 1])
    arrived(txt.at[core, y, pl.ds(0, NX - 1)], text_send.at[0])

    @pl.when(zl != core)
    def _():
        arrived(txt.at[core, y, 0], text_send.at[3])

    arrived(txt.at[core, pl.ds(0, NY - 1)], text_send.at[1])
    arrived(txt.at[core], text_send.at[2])
    keep(ob, rs, own_b, 0).wait()
    keep(od, rc, own_b, 1).wait()
    keep(oc.at[NX - 1], rc, own_a, 2).wait()
    keep(oa.at[NX - 1], rs, own_a, 3).wait()
    for n, r in enumerate((rs, rc)):
        moved = r.at[pl.ds(0, (others + NZ * NC - 1) // 2)]
        arrived(moved, out_recv.at[n])
        arrived(moved, out_send.at[n])


def block(pad, q, k, v, c, text_key, text_value):
    any_spec = pl.BlockSpec(memory_space=pl.ANY)
    vmem = pl.BlockSpec(memory_space=pltpu.VMEM)
    dma = pltpu.SemaphoreType.DMA
    half = lambda *s: pltpu.VMEM(s, jnp.bfloat16)
    full = lambda *s: pltpu.VMEM(s, jnp.float32)
    landing = [REGION, REGION, SPAN, SPAN, REGION, REGION, SPAN, SPAN]
    result = jax.ShapeDtypeStruct((HEADS, NC, PAD, HD), jnp.bfloat16)
    return pl.pallas_call(
        block_kernel,
        in_specs=[pl.BlockSpec(memory_space=pltpu.SMEM)] + [vmem] * 3 + [any_spec] * 6,
        out_specs=[any_spec] * 10,
        out_shape=[result] * 2 + [jax.ShapeDtypeStruct((n, HD), jnp.bfloat16) for n in landing],
        scratch_shapes=[
            half(TOK, HEADS * HD), half(TOK, HEADS * HD), half(HEADS, TOK, HD), half(HEADS, TOK, HD),
            half(REGION, HD), half(NX, WIDE, HD), half(REGION, HD), half(WIDE, HD),
            half(NC * NY, REGION, HD), half(NC * NY, REGION, HD), half(NC, NY, SPAN, HD), half(NC, NY, SPAN, HD),
            half(NC, NY, NX, 2, 2, 16, HD),
            full(REGION, WIDE), full(REGION, WIDE), half(HD, REGION), half(4, HD, REGION), full(HD, NX * WIDE),
            full(8, NX * WIDE), full(8, NX * WIDE), half(HD, REGION),
            half(NX, GROUPS, PAD, HD), half(GROUPS, PAD, HD), half(NX, GROUPS, PAD, HD), half(GROUPS, PAD, HD),
            half(2 * NX, HD, WIDE), full(2 * NX, 8, WIDE),
            dma((4,)), dma((8,)), dma((10,)), dma((8, 2)), dma((8, 2)), dma((5, 2)), dma((5, 2)), dma((3,)), dma((3,)),
            dma((3, 2)), dma((3, 2)), dma((4,)), dma((3,)), dma((2,)), dma((2,)), dma((4,)),
        ],
        compiler_params=pltpu.CompilerParams(collective_id=0, has_side_effects=True),
        name="block",
    )(pad, omega_table(), order_matrix(), frame_cells(), q, k, v, c, text_key, text_value)[:2]


def frame_cells():
    z, i, j = np.meshgrid(np.arange(NZ), np.arange(TH), np.arange(TW), indexing="ij")
    cells = (z % 2) * TH * GRID_W + i * GRID_W + (z // 2) * 2 * TW + j
    return jnp.asarray(np.broadcast_to(cells.reshape(-1, 1), (SPAN, HD)), jnp.int32)


def order_matrix():
    perm = np.zeros((GROUPS * PAD, NZ * TOK), np.float32)
    for zl in range(2):
        for a in range(2):
            for i in range(TH):
                for zh2 in range(2):
                    for j in range(TW):
                        row = (zl * 8 + a * 4 + i) * PAD + zh2 * TW + j
                        perm[row, (2 * (2 * a + zh2) + zl) * TOK + i * TW + j] = 1
    return jnp.asarray(perm, jnp.bfloat16)


def omega_table():
    pair = np.arange(HD) // 2
    side = HD // 6
    first = HD // 2 - 2 * side
    table = np.zeros((8, HD), np.float32)
    for axis, start, count in ((0, 0, first), (1, first, side), (2, first + side, side)):
        inside = (pair >= start) & (pair < start + count)
        table[axis] = np.where(inside, 10000.0 ** (-((pair - start) / count)), 0.0)
    table[3] = np.where(np.arange(HD) % 2 == 0, -1.0, 1.0)
    return jnp.asarray(table)


def body(self_query, self_key, self_value, cross_query, text_key, text_value, padded_count):
    results = block(padded_count, self_query, self_key, self_value, cross_query, text_key, text_value)

    def finish(r):
        r = r[:, :, : 2 * TW].reshape(HEADS, NC, 2, TW, HD)
        return r.transpose(2, 1, 3, 0, 4).reshape(TOK, HEADS * HD)

    return finish(results[0]), finish(results[1])


def solution(mesh):
    split = Mesh(mesh.devices.reshape(4, 4, 2, 4, 2), BLK + ULY)
    own = P(BLK + ULY, None)
    return jax.shard_map(body, mesh=split, in_specs=(own,) * 4 + (P(BLK, ULY),) * 2 + (P(),),
                         out_specs=(own, own), check_vma=False)
```

```python
import functools
import math

import jax
import jax.numpy as jnp
import numpy as np
from jax import lax
from jax.experimental import pallas as pl
from jax.experimental.pallas import tpu as pltpu
from jax.sharding import Mesh
from jax.sharding import PartitionSpec as P

HD = 128
TH = 4
TW = 10
TOK = TH * TW
ROW_TILES = 8
NX, NY, NZ, NC = 4, 4, 8, 2
LAYER = 5
HEADS = NZ * LAYER
GRID_H = TH * ROW_TILES
GRID_W = TW * NZ
KEYS = NX * NY * NZ * NC * TOK
TEXT = 512
LAST = KEYS // NX
PIECE = 2 * TW
PAD = 24
GROUPS = 16
ULY = ("uly_0", "uly_1")
BLK = ("blk_0", "blk_1", "blk_2")
NEG = -1e30
MESH = pl.DeviceIdType.MESH


def place():
    x = lax.axis_index("blk_0")
    y = lax.axis_index("blk_1")
    z = lax.axis_index("uly_0") * 2 + lax.axis_index("blk_2")
    return x, y, z, lax.axis_index("uly_1")


def at_xz(x, z):
    return {"blk_0": x, "uly_0": z // 2, "blk_2": lax.rem(z, 2)}


SPAN = NZ * TOK
REGION = NX * SPAN
WIDE = 384
TILE = 256
SCALE = math.log2(math.e) / math.sqrt(HD)
NT = (((1,), (1,)), ((), ()))


def block_kernel(
    pad_ref, omegas, perm, place_in_frame, q_hbm, k_hbm, v, c, text_key, text_value,
    out_s, out_c, qa_h, ca_h, qb_h, cb_h, ka_h, va_h, kb_h, vb_h,
    rs, rc, q_in, k_in, q, k, qa, qb, ca, cb, ka, va, kb, vb, txt, s0, s1, vt, vt4, acc, row_m, row_l, ot, oa, ob, oc, od, part, stat,
    send, recv, local, ring_send, ring_recv, twin_send, twin_recv, fan_send, fan_recv, part_send, part_recv,
    text_send, text_recv, out_send, out_recv, near,
):
    x, y, z, core = place()
    zl, zh = lax.axis_index("blk_2"), lax.axis_index("uly_0")
    twin = {"uly_1": 1 - core}
    yp, ym, yo = lax.rem(y + 1, NY), lax.rem(y + NY - 1, NY), lax.rem(y + 2, NY)
    others = NX * NZ * NC - 1

    def owner(n, m):
        ti = lax.rem(zh + m // 4, 4)
        tl = lax.rem(zl + lax.rem(m // 2, 2), 2)
        ta = lax.rem(core + lax.rem(m, 2), 2)
        peer = {"blk_0": lax.rem(x + n, NX), "uly_0": ti, "blk_2": tl, "uly_1": ta}
        return tl * 8 + ta * 4 + ti, peer

    loads = [pltpu.make_async_copy(k_hbm, k_in, local.at[8]), pltpu.make_async_copy(q_hbm, q_in, local.at[9])]
    for load in loads:
        load.start()
    barrier = pltpu.get_barrier_semaphore()

    for n in (2, 1, 3, 0):
        for zz in (2, 1, 3, 0):
            for m in range(4):
                if (n, zz, m) != (0, 0, 0):
                    peer = owner(n, zz * 4 + m)[1]
                    pl.semaphore_signal(barrier, inc=1, device_id=peer, device_id_type=MESH)
    for yy in (yp, ym, yo):
        pl.semaphore_signal(barrier, inc=1, device_id={"blk_1": yy}, device_id_type=MESH)

    token = lax.broadcasted_iota(jnp.int32, (TOK, HD), 0)
    chunk = (x * NY + y) * 2 + zl
    row = lax.rem(chunk, ROW_TILES) * TH + token // TW
    col = (zh * 2 + core) * TW + lax.rem(token, TW)
    angles = (jnp.full((TOK, HD), chunk // ROW_TILES).astype(jnp.float32) * omegas[0:1, :]
              + row.astype(jnp.float32) * omegas[1:2, :] + col.astype(jnp.float32) * omegas[2:3, :])
    cos, sin = jnp.cos(angles), jnp.sin(angles) * omegas[3:4, :]
    for load in loads:
        load.wait()
    even = lax.rem(lax.broadcasted_iota(jnp.int32, (TOK, HD), 1), 2) == 0

    def rotate(n, carry):
        for src, dst in ((k_in, k), (q_in, q)):
            for h in range(LAYER):
                wide = src[:, pl.ds(pl.multiple_of((n * LAYER + h) * HD, HD), HD)].astype(jnp.float32)
                partner = jnp.where(even, pltpu.roll(wide, HD - 1, 1), pltpu.roll(wide, 1, 1))
                dst[n * LAYER + h] = (wide * cos + partner * sin).astype(jnp.bfloat16)
        return carry

    lax.fori_loop(0, NZ, rotate, 0)
    pl.semaphore_wait(barrier, others + 3)

    def channels(ref, h):
        return ref.at[:, pl.ds(pl.multiple_of(h * HD, HD), HD)]

    def of_head(ref, h):
        return channels(ref, h) if ref is v or ref is c else ref.at[h]

    def arrived(ref, sem):
        pltpu.make_async_copy(ref, ref, sem).wait()

    def push(src, dst, s, r, peer):
        pltpu.make_async_remote_copy(src, dst, s, r, device_id=peer, device_id_type=MESH).start()

    own_a, own_b = z * LAYER + x, z * LAYER + LAYER - 1

    def rows(ref, start):
        return ref.at[pl.ds(pl.multiple_of(start, 8), TOK)]

    def rows_of(n):
        return n * SPAN + z * TOK

    def send_b(pairs):
        def run(n, carry):
            tz = lax.rem(z + n, NZ)
            h, peer = tz * LAYER + LAYER - 1, at_xz(x, tz)
            for s, src, r, dst in pairs:
                push(of_head(src, h), rows(dst, z * TOK), send.at[s], recv.at[r], peer)
            return carry
        for s, src, r, dst in pairs:
            pltpu.make_async_copy(of_head(src, own_b), rows(dst, z * TOK), recv.at[r]).start()
        lax.fori_loop(1, NZ, run, 0)

    def send_a(pairs, relative):
        def where(tx):
            return rows_of(lax.rem(x - tx + NX + NX - 1, NX)) if relative else rows_of(x)
        def run(n, carry):
            tx, tz = lax.rem(x + n // NZ, NX), lax.rem(z + lax.rem(n, NZ), NZ)
            h, peer = tz * LAYER + tx, at_xz(tx, tz)
            for s, src, r, dst in pairs:
                push(of_head(src, h), rows(dst, where(tx)), send.at[s], recv.at[r], peer)
            return carry
        for s, src, r, dst in pairs:
            pltpu.make_async_copy(of_head(src, own_a), rows(dst, where(x)), recv.at[r]).start()
        lax.fori_loop(1, NX * NZ, run, 0)

    send_b(((2, k, 0, kb_h), (3, v, 1, vb_h), (0, q, 2, qb_h)))
    def text_pieces(n):
        tx = lax.rem(x + n, NX)
        for ab, h in ((0, tx), (1, LAYER - 1)):
            for t, src in enumerate((text_key, text_value)):
                yield channels(src, h), txt.at[zl, y, x, ab, t], {"blk_0": tx, "blk_2": core, "uly_1": zl}

    for n in range(1, NX):
        for src, dst, peer in text_pieces(n):
            push(src, dst, text_send.at[0], text_recv.at[0], peer)

    @pl.when(zl != core)
    def _():
        for src, dst, peer in text_pieces(0):
            push(src, dst, text_send.at[3], text_recv.at[0], peer)

    @pl.when(zl == core)
    def _():
        for src, dst, peer in text_pieces(0):
            pltpu.make_async_copy(src, dst, text_recv.at[0]).start()

    send_a(((2, k, 3, ka_h),), False)
    send_a(((3, v, 4, va_h),), False)
    send_a(((0, q, 5, qa_h),), True)
    send_b(((1, c, 6, cb_h),))
    send_a(((1, c, 7, ca_h),), True)

    qb[:, SPAN:, :] = jnp.zeros((NX, WIDE - SPAN, HD), jnp.bfloat16)
    cb[SPAN:, :] = jnp.zeros((WIDE - SPAN, HD), jnp.bfloat16)
    row_m[...] = jnp.full_like(row_m, NEG)
    row_l[...] = jnp.zeros_like(row_l)
    acc[...] = jnp.zeros_like(acc)
    stat[...] = jnp.zeros_like(stat)

    def give(kind, region, target, n, which=(0, 1)):
        for t in which:
            push(region(kind[t]), region(kind[t]), ring_send.at[n, t], ring_recv.at[n, t], {"blk_1": target})

    def took(kind, region, n, which=(0, 1)):
        for t in which:
            arrived(region(kind[t]), ring_recv.at[n, t])

    def share(kind, region, n, which=(0, 1)):
        for t in which:
            push(region(kind[t]), region(kind[t]), twin_send.at[n, t], twin_recv.at[n, t], twin)

    def land(src, dst, r, n):
        arrived(src, recv.at[r])
        pltpu.make_async_copy(src, dst, local.at[n]).start()
        return lambda: pltpu.make_async_copy(src, dst, local.at[n]).wait()

    a, b = (ka, va), (kb, vb)
    mine = core * NY
    a_y = lambda yy: lambda r: r.at[mine + yy]
    a_half = lambda yy, s: lambda r: r.at[mine + yy, pl.ds(s * (REGION // 2), REGION // 2)]
    b_y = lambda yy: lambda r: r.at[core, yy]
    b_half = lambda yy, s: lambda r: r.at[core, yy, pl.ds(s * (SPAN // 2), SPAN // 2)]
    b_all = lambda r: r.at[core]

    for done in [land(kb_h, kb.at[core, y], 0, 0), land(vb_h, vb.at[core, y], 1, 1)]:
        done()
    give(b, b_y(y), yp, 0)
    give(b, b_y(y), ym, 1)
    land(qb_h, qb.at[0, pl.ds(0, SPAN)], 2, 2)()
    for n in range(1, NX):
        push(qb.at[0, pl.ds(0, SPAN)], qb.at[NX - n, pl.ds(0, SPAN)], fan_send.at[n - 1], fan_recv.at[NX - n - 1],
             {"blk_0": lax.rem(x + n, NX)})
    arrived(txt.at[core, y], text_recv.at[0])
    for yy in (yp, ym, yo):
        push(txt.at[core, y], txt.at[core, y], text_send.at[1], text_recv.at[1], {"blk_1": yy})
    took(b, b_y(ym), 0)
    give(b, b_half(ym, 0), yp, 2)
    took(b, b_y(yp), 1)
    give(b, b_half(yp, 1), ym, 3)
    took(b, b_half(yo, 0), 2)
    took(b, b_half(yo, 1), 3)
    share(b, b_all, 4)
    arrived(txt.at[core, pl.ds(0, NY - 1)], text_recv.at[1])
    push(txt.at[core], txt.at[core], text_send.at[2], text_recv.at[2], twin)
    for n in range(1, NX):
        arrived(qb.at[n, pl.ds(0, SPAN)], fan_recv.at[n - 1])

    held = (s0, s1)

    def absorb(cols, width, s, peak, values):
        m = row_m[0:1, cols]
        new = jnp.maximum(m, peak)
        shrink = jnp.exp2((m - new) * SCALE)
        p = jnp.exp2((s[:, :width] - new) * SCALE)
        row_m[0:1, cols] = new
        row_l[0:1, cols] = row_l[0:1, cols] * shrink + jnp.sum(p, axis=0, keepdims=True)
        acc[:, cols] = acc[:, cols] * shrink + jnp.dot(
            values[...], p.astype(jnp.bfloat16), preferred_element_type=jnp.float32)

    def attend(queries, width, scores):
        peaks = scores(queries[0][0], s0)
        for n, (_, cols) in enumerate(queries):
            ahead = scores(queries[n + 1][0], held[(n + 1) % 2]) if n + 1 < len(queries) else None
            absorb(cols, width, held[n % 2], peaks, vt)
            peaks = ahead

    limit = KEYS - (NX - 1) * LAST - pad_ref[0]
    limit_b = jnp.where(x == NX - 1, limit, LAST)

    def masked(s, cc, yy, bound):
        cells = jnp.concatenate([place_in_frame[...]] * (s.shape[1] // HD), axis=1)
        return jnp.where(cells < bound - yy * (2 * TH * GRID_W) - cc * TW, s, NEG)

    def own_region(t):
        land((ka_h, va_h)[t], a[t].at[mine + y], 3 + t, 3 + t)()
        give(a, a_y(y), yp, 4, (t,))
        give(a, a_y(y), ym, 5, (t,))
        share(a, a_y(y), 0, (t,))

    def pass_on(t):
        took(a, a_y(ym), 4, (t,))
        give(a, a_half(ym, 0), yp, 6, (t,))
        share(a, a_y(ym), 1, (t,))
        took(a, a_y(yp), 5, (t,))
        give(a, a_half(yp, 1), ym, 7, (t,))
        share(a, a_y(yp), 2, (t,))

    b_tiles = [(n, slice(n * WIDE, (n + 1) * WIDE)) for n in range(NX)]

    def b_region(i, carry):
        cc = lax.rem(core + i, NC)

        @pl.when(i == 1)
        def _():
            for t in range(2):
                arrived(b[t].at[1 - core], twin_recv.at[4, t])

        vt[...] = vb[cc].reshape(REGION, HD).T

        def scores(n, into):
            s = lax.dot_general(kb[cc].reshape(REGION, HD), qb[n], NT, preferred_element_type=jnp.float32)
            peak = jnp.full((1, WIDE), NEG, jnp.float32)
            for yy in range(NY):
                cut = slice(yy * SPAN, (yy + 1) * SPAN)
                e = masked(s[cut], cc, yy, limit_b)
                into[cut, :] = e
                peak = jnp.maximum(peak, jnp.max(e, axis=0, keepdims=True))
            return peak

        attend(b_tiles, WIDE, scores)
        return carry

    own_region(0)
    lax.fori_loop(0, NC, b_region, 0)
    for n in range(NX):
        cols = slice(n * WIDE, (n + 1) * WIDE)
        part[n] = (acc[:, cols] / row_l[0:1, cols]).astype(jnp.bfloat16)
        stat[n, 0:1, :] = row_m[0:1, cols]
        stat[n, 1:2, :] = row_l[0:1, cols]
    for n in range(1, NX):
        peer = {"blk_0": lax.rem(x + n, NX)}
        push(part.at[n], part.at[NX + n], part_send.at[n - 1, 0], part_recv.at[n - 1, 0], peer)
        push(stat.at[n], stat.at[NX + n], part_send.at[n - 1, 1], part_recv.at[n - 1, 1], peer)

    row_m[...] = jnp.full_like(row_m, NEG)
    row_l[...] = jnp.zeros_like(row_l)
    acc[...] = jnp.zeros_like(acc)

    own_region(1)
    pass_on(0)

    def ordered(cols):
        return lax.dot_general(perm[...], cols, NT, preferred_element_type=jnp.float32).reshape(
            GROUPS, PAD, HD)[:, :PIECE].astype(jnp.bfloat16)

    def landing(result, head):
        return result.at[core, :, pl.ds(pl.multiple_of(head * HD, HD), HD)]

    def deliver(src, result, n, head, which):
        for m in range(1 if n == 0 else 0, GROUPS):
            g, peer = owner(n, m)
            push(src.at[g], landing(result, head), out_send.at[which], out_recv.at[which], peer)

    def keep(src, result, head, n):
        return pltpu.make_async_copy(src.at[zl * 8 + core * 4 + zh], landing(result, head), near.at[n])

    a_tiles = [(slice(n * TILE, (n + 1) * TILE),) * 2 for n in range(REGION // TILE)]

    def text_rows(ab, kv):
        return txt[:, :, :, ab, kv].reshape(-1, HD)

    def text_scores(q_tile, keys, into):
        s = lax.dot_general(keys, q_tile, NT, preferred_element_type=jnp.float32)
        into[:TEXT, : q_tile.shape[0]] = s
        return jnp.max(s, axis=0, keepdims=True)

    def text_mix(s, width, peak, values_t):
        p = jnp.exp2((s[:TEXT, :width] - peak) * SCALE)
        weighted = jnp.dot(values_t, p.astype(jnp.bfloat16), preferred_element_type=jnp.float32)
        return (weighted / jnp.sum(p, axis=0, keepdims=True)).astype(jnp.bfloat16)

    def merge_parts():
        for n in range(1, NX):
            arrived(part.at[NX + n], part_recv.at[n - 1, 0])
            arrived(stat.at[NX + n], part_recv.at[n - 1, 1])
        slots = [0] + [NX + n for n in range(1, NX)]
        top = stat[0, 0:1, :]
        for n in slots[1:]:
            top = jnp.maximum(top, stat[n, 0:1, :])
        weights = [stat[n, 1:2, :] * jnp.exp2((stat[n, 0:1, :] - top) * SCALE) for n in slots]
        total = weights[0] + weights[1] + weights[2] + weights[3]
        merged = part[0].astype(jnp.float32) * (weights[0] / total)
        for n, w in zip(slots[1:], weights[1:]):
            merged = merged + part[n].astype(jnp.float32) * (w / total)
        ob[...] = ordered(merged.astype(jnp.bfloat16)[:, :SPAN])
        keep(ob, rs, own_b, 0).start()
        deliver(ob, rs, 0, own_b, 0)

    def attend_text():
        arrived(txt.at[1 - core], text_recv.at[2])
        land(cb_h, cb.at[pl.ds(0, SPAN)], 6, 6)()
        land(ca_h, ca, 7, 7)()
        keys_b, values_b = text_rows(1, 0), text_rows(1, 1).T
        keys, values_t = text_rows(0, 0), text_rows(0, 1).T
        peak_b = text_scores(cb[...], keys_b, s0)
        peak = text_scores(ca[a_tiles[0][0], :], keys, s1)
        result_b = text_mix(s0, WIDE, peak_b, values_b)
        for n, (cols, _) in enumerate(a_tiles):
            if n + 1 < len(a_tiles):
                ahead = text_scores(ca[a_tiles[n + 1][0], :], keys, held[n % 2])
            ot[:, cols] = text_mix(held[(n + 1) % 2], TILE, peak, values_t)
            peak = ahead
            if n > 0:
                oc[n - 1] = ordered(ot[:, (n - 1) * SPAN : n * SPAN])
                deliver(oc.at[n - 1], rc, n % NX, own_a, 1)
        keep(oc.at[NX - 1], rc, own_a, 2).start()
        od[...] = ordered(result_b[:, :SPAN])
        keep(od, rc, own_b, 1).start()
        deliver(od, rc, 0, own_b, 1)

    def region_of(i):
        theirs = jnp.logical_or(i == 1, jnp.logical_or(jnp.logical_or(i == 4, i == 5), i == 7))
        cc = jnp.where(theirs, 1 - core, core)
        yy = jnp.where(i < 2, y, jnp.where(i >= 6, yo, jnp.where(lax.rem(i, 2) == 0, ym, yp)))
        return cc, yy, cc * NY + yy

    def a_scores(region, cols, into):
        cc, yy, at = region
        q_tile = qa[cols, :]
        s = lax.dot_general(ka[at, : REGION - SPAN, :], q_tile, NT, preferred_element_type=jnp.float32)
        into[: REGION - SPAN, :TILE] = s
        e = lax.dot_general(ka[at, REGION - SPAN :, :], q_tile, NT, preferred_element_type=jnp.float32)
        e = masked(e, cc, yy, limit)
        into[REGION - SPAN :, :TILE] = e
        return jnp.maximum(jnp.max(s, axis=0, keepdims=True), jnp.max(e, axis=0, keepdims=True))

    def a_region(i, carry):
        region = region_of(i)

        @pl.when(i == 1)
        def _():
            for t in range(2):
                arrived(a[t].at[region[2]], twin_recv.at[0, t])

        @pl.when(i == 2)
        def _():
            pass_on(1)
            merge_parts()

        @pl.when(i == 3)
        def _():
            attend_text()

        vt[...] = va[region[2]].T
        attend(a_tiles, TILE, lambda cols, into: a_scores(region, cols, into))
        return carry

    land(qa_h, qa, 5, 5)()
    lax.fori_loop(0, 4, a_region, 0)
    took(a, a_half(yo, 0), 6)
    took(a, a_half(yo, 1), 7)
    share(a, a_y(yo), 3)

    last = [region_of(i) for i in (4, 5, 6, 7)]
    for (cc, yy, at), n in ((last[0], 1), (last[1], 2), (last[3], 3)):
        for t in range(2):
            arrived(a[t].at[at], twin_recv.at[n, t])
    for n, region in enumerate(last):
        vt4[n] = va[region[2]].T

    def a_tile(t, peak):
        cols = pl.ds(pl.multiple_of(t * TILE, TILE), TILE)
        after = pl.ds(pl.multiple_of(jnp.minimum(t + 1, REGION // TILE - 1) * TILE, TILE), TILE)
        for n in range(4):
            if n < 3:
                ahead = a_scores(last[n + 1], cols, held[(n + 1) % 2])
            else:
                ahead = a_scores(last[0], after, held[0])
            absorb(cols, TILE, held[n % 2], peak, vt4.at[n])
            peak = ahead
        ot[:, cols] = (acc[:, cols] / row_l[0:1, cols]).astype(jnp.bfloat16)
        for n in range(NX):
            @pl.when(t == n + 1)
            def _():
                oa[n] = ordered(ot[:, n * SPAN : (n + 1) * SPAN])
                if n == NX - 1:
                    keep(oa.at[n], rs, own_a, 3).start()
                deliver(oa.at[n], rs, (n + 1) % NX, own_a, 0)
        return peak

    lax.fori_loop(0, REGION // TILE, a_tile, a_scores(last[0], slice(0, TILE), held[0]))

    for n in range(4):
        arrived(v.at[:, pl.ds(0, (NX * NZ - 1 + NZ - 1) * HD)], send.at[n])
    for t in range(2):
        for n in (0, 1):
            arrived(b_y(y)(b[t]), ring_send.at[n, t])
            arrived(b_half(y, 0)(b[t]), ring_send.at[2 + n, t])
            arrived(a_y(y)(a[t]), ring_send.at[4 + n, t])
            arrived(a_half(y, 0)(a[t]), ring_send.at[6 + n, t])
        for n in range(4):
            arrived(a_y(y)(a[t]), twin_send.at[n, t])
        arrived(b[t].at[core], twin_send.at[4, t])
    for n in range(1, NX):
        arrived(qb.at[n, pl.ds(0, SPAN)], fan_send.at[n - 1])
        arrived(part.at[n], part_send.at[n - 1, 0])
        arrived(stat.at[n], part_send.at[n - 1, 1])
    arrived(txt.at[core, y, pl.ds(0, NX - 1)], text_send.at[0])

    @pl.when(zl != core)
    def _():
        arrived(txt.at[core, y, 0], text_send.at[3])

    arrived(txt.at[core, pl.ds(0, NY - 1)], text_send.at[1])
    arrived(txt.at[core], text_send.at[2])
    keep(ob, rs, own_b, 0).wait()
    keep(od, rc, own_b, 1).wait()
    keep(oc.at[NX - 1], rc, own_a, 2).wait()
    keep(oa.at[NX - 1], rs, own_a, 3).wait()
    for n, r, out in ((1, rc, out_c), (0, rs, out_s)):
        moved = r.at[:, :, pl.ds(0, (others + NZ * NC - 1) // 2 * HD)]
        arrived(moved, out_recv.at[n])
        out[...] = sum(jnp.dot(rows_to_own(cc), r[cc], preferred_element_type=jnp.float32)
                       for cc in range(NC)).astype(jnp.bfloat16)
        arrived(moved, out_send.at[n])


def rows_to_own(core):
    to = lax.broadcasted_iota(jnp.int32, (TOK, PIECE), 0)
    piece = lax.broadcasted_iota(jnp.int32, (TOK, PIECE), 1)
    return jnp.where(to == piece + (piece // TW) * TW + core * TW, 1.0, 0.0).astype(jnp.bfloat16)


def block(pad, q, k, v, c, text_key, text_value):
    any_spec = pl.BlockSpec(memory_space=pl.ANY)
    vmem = pl.BlockSpec(memory_space=pltpu.VMEM)
    dma = pltpu.SemaphoreType.DMA
    half = lambda *s: pltpu.VMEM(s, jnp.bfloat16)
    full = lambda *s: pltpu.VMEM(s, jnp.float32)
    landing = [REGION, REGION, SPAN, SPAN, REGION, REGION, SPAN, SPAN]
    result = jax.ShapeDtypeStruct((TOK, HEADS * HD), jnp.bfloat16)
    return pl.pallas_call(
        block_kernel,
        in_specs=[pl.BlockSpec(memory_space=pltpu.SMEM)] + [vmem] * 3 + [any_spec] * 6,
        out_specs=[vmem] * 2 + [any_spec] * 8,
        out_shape=[result] * 2 + [jax.ShapeDtypeStruct((n, HD), jnp.bfloat16) for n in landing],
        scratch_shapes=[
            half(NC, PIECE, HEADS * HD), half(NC, PIECE, HEADS * HD),
            half(TOK, HEADS * HD), half(TOK, HEADS * HD), half(HEADS, TOK, HD), half(HEADS, TOK, HD),
            half(REGION, HD), half(NX, WIDE, HD), half(REGION, HD), half(WIDE, HD),
            half(NC * NY, REGION, HD), half(NC * NY, REGION, HD), half(NC, NY, SPAN, HD), half(NC, NY, SPAN, HD),
            half(NC, NY, NX, 2, 2, 16, HD),
            full(REGION, WIDE), full(REGION, WIDE), half(HD, REGION), half(4, HD, REGION), full(HD, NX * WIDE),
            full(8, NX * WIDE), full(8, NX * WIDE), half(HD, REGION),
            half(NX, GROUPS, PIECE, HD), half(GROUPS, PIECE, HD), half(NX, GROUPS, PIECE, HD), half(GROUPS, PIECE, HD),
            half(2 * NX, HD, WIDE), full(2 * NX, 8, WIDE),
            dma((4,)), dma((8,)), dma((10,)), dma((8, 2)), dma((8, 2)), dma((5, 2)), dma((5, 2)), dma((3,)), dma((3,)),
            dma((3, 2)), dma((3, 2)), dma((4,)), dma((3,)), dma((2,)), dma((2,)), dma((4,)),
        ],
        compiler_params=pltpu.CompilerParams(collective_id=0, has_side_effects=True),
        name="block",
    )(pad, omega_table(), order_matrix(), frame_cells(), q, k, v, c, text_key, text_value)[:2]


def frame_cells():
    z, i, j = np.meshgrid(np.arange(NZ), np.arange(TH), np.arange(TW), indexing="ij")
    cells = (z % 2) * TH * GRID_W + i * GRID_W + (z // 2) * 2 * TW + j
    return jnp.asarray(np.broadcast_to(cells.reshape(-1, 1), (SPAN, HD)), jnp.int32)


def order_matrix():
    perm = np.zeros((GROUPS * PAD, NZ * TOK), np.float32)
    for zl in range(2):
        for a in range(2):
            for i in range(TH):
                for zh2 in range(2):
                    for j in range(TW):
                        row = (zl * 8 + a * 4 + i) * PAD + zh2 * TW + j
                        perm[row, (2 * (2 * a + zh2) + zl) * TOK + i * TW + j] = 1
    return jnp.asarray(perm, jnp.bfloat16)


def omega_table():
    pair = np.arange(HD) // 2
    side = HD // 6
    first = HD // 2 - 2 * side
    table = np.zeros((8, HD), np.float32)
    for axis, start, count in ((0, 0, first), (1, first, side), (2, first + side, side)):
        inside = (pair >= start) & (pair < start + count)
        table[axis] = np.where(inside, 10000.0 ** (-((pair - start) / count)), 0.0)
    table[3] = np.where(np.arange(HD) % 2 == 0, -1.0, 1.0)
    return jnp.asarray(table)


def body(self_query, self_key, self_value, cross_query, text_key, text_value, padded_count):
    return tuple(block(padded_count, self_query, self_key, self_value, cross_query, text_key, text_value))


def solution(mesh):
    split = Mesh(mesh.devices.reshape(4, 4, 2, 4, 2), BLK + ULY)
    own = P(BLK + ULY, None)
    return jax.shard_map(body, mesh=split, in_specs=(own,) * 4 + (P(BLK, ULY),) * 2 + (P(),),
                         out_specs=(own, own), check_vma=False)
```

```python
import functools
import math

import jax
import jax.numpy as jnp
import numpy as np
from jax import lax
from jax.experimental import pallas as pl
from jax.experimental.pallas import tpu as pltpu
from jax.sharding import Mesh
from jax.sharding import PartitionSpec as P

HD = 128
TH = 4
TW = 10
TOK = TH * TW
ROW_TILES = 8
NX, NY, NZ, NC = 4, 4, 8, 2
LAYER = 5
HEADS = NZ * LAYER
GRID_H = TH * ROW_TILES
GRID_W = TW * NZ
KEYS = NX * NY * NZ * NC * TOK
TEXT = 512
LAST = KEYS // NX
PIECE = 2 * TW
PAD = 24
GROUPS = 16
ULY = ("uly_0", "uly_1")
BLK = ("blk_0", "blk_1", "blk_2")
NEG = -1e30
MESH = pl.DeviceIdType.MESH


def place():
    x = lax.axis_index("blk_0")
    y = lax.axis_index("blk_1")
    z = lax.axis_index("uly_0") * 2 + lax.axis_index("blk_2")
    return x, y, z, lax.axis_index("uly_1")


def at_xz(x, z):
    return {"blk_0": x, "uly_0": z // 2, "blk_2": lax.rem(z, 2)}


SPAN = NZ * TOK
REGION = NX * SPAN
WIDE = 384
TILE = 256
SCALE = math.log2(math.e) / math.sqrt(HD)
NT = (((1,), (1,)), ((), ()))


def block_kernel(
    pad_hbm, omegas_hbm, q_hbm, k_hbm, v, c, text_key, text_value,
    out_s, out_c, qa_h, ca_h, qb_h, cb_h, ka_h, va_h, kb_h, vb_h,
    pad_ref, omegas, perm, place_in_frame, rs, rc, q_in, k_in, q, k, qa, qb, ca, cb, ka, va, kb, vb, txt, s0, s1, vt, vt4, acc, row_m, row_l, ot, oa, ob, oc, od, part, stat,
    send, recv, local, ring_send, ring_recv, twin_send, twin_recv, fan_send, fan_recv, part_send, part_recv,
    text_send, text_recv, out_send, out_recv, near,
):
    x, y, z, core = place()
    zl, zh = lax.axis_index("blk_2"), lax.axis_index("uly_0")
    twin = {"uly_1": 1 - core}
    yp, ym, yo = lax.rem(y + 1, NY), lax.rem(y + NY - 1, NY), lax.rem(y + 2, NY)
    others = NX * NZ * NC - 1

    def owner(n, m):
        ti = lax.rem(zh + m // 4, 4)
        tl = lax.rem(zl + lax.rem(m // 2, 2), 2)
        ta = lax.rem(core + lax.rem(m, 2), 2)
        peer = {"blk_0": lax.rem(x + n, NX), "uly_0": ti, "blk_2": tl, "uly_1": ta}
        return tl * 8 + ta * 4 + ti, peer

    loads = [pltpu.make_async_copy(src, dst, local.at[8 + n]) for n, (src, dst) in enumerate(
        ((k_hbm, k_in), (q_hbm, q_in), (omegas_hbm, omegas), (pad_hbm, pad_ref)))]
    for load in loads:
        load.start()
    barrier = pltpu.get_barrier_semaphore()

    for n in (2, 1, 3, 0):
        for zz in (2, 1, 3, 0):
            for m in range(4):
                if (n, zz, m) != (0, 0, 0):
                    peer = owner(n, zz * 4 + m)[1]
                    pl.semaphore_signal(barrier, inc=1, device_id=peer, device_id_type=MESH)
    for yy in (yp, ym, yo):
        pl.semaphore_signal(barrier, inc=1, device_id={"blk_1": yy}, device_id_type=MESH)

    n = lax.broadcasted_iota(jnp.int32, (SPAN, HD), 0)
    n_z, n_t = n // TOK, lax.rem(n, TOK)
    place_in_frame[...] = (lax.rem(n_z, 2) * TH + n_t // TW) * GRID_W + (n_z // 2) * (2 * TW) + lax.rem(n_t, TW)
    to = lax.broadcasted_iota(jnp.int32, (GROUPS * PAD, SPAN), 0)
    at = lax.broadcasted_iota(jnp.int32, (GROUPS * PAD, SPAN), 1)
    g, r = to // PAD, lax.rem(to, PAD)
    wanted = ((2 * (2 * (lax.rem(g, 8) // TH) + r // TW) + g // 8) * TOK + lax.rem(g, TH) * TW + lax.rem(r, TW))
    perm[...] = jnp.where(jnp.logical_and(at == wanted, r < PIECE), 1.0, 0.0).astype(jnp.bfloat16)

    for load in loads:
        load.wait()
    token = lax.broadcasted_iota(jnp.int32, (TOK, HD), 0)
    chunk = (x * NY + y) * 2 + zl
    row = lax.rem(chunk, ROW_TILES) * TH + token // TW
    col = (zh * 2 + core) * TW + lax.rem(token, TW)
    angles = (jnp.full((TOK, HD), chunk // ROW_TILES).astype(jnp.float32) * omegas[0:1, :]
              + row.astype(jnp.float32) * omegas[1:2, :] + col.astype(jnp.float32) * omegas[2:3, :])
    cos, sin = jnp.cos(angles), jnp.sin(angles) * omegas[3:4, :]
    even = lax.rem(lax.broadcasted_iota(jnp.int32, (TOK, HD), 1), 2) == 0

    def rotate(n, carry):
        for src, dst in ((k_in, k), (q_in, q)):
            for h in range(LAYER):
                wide = src[:, pl.ds(pl.multiple_of((n * LAYER + h) * HD, HD), HD)].astype(jnp.float32)
                partner = jnp.where(even, pltpu.roll(wide, HD - 1, 1), pltpu.roll(wide, 1, 1))
                dst[n * LAYER + h] = (wide * cos + partner * sin).astype(jnp.bfloat16)
        return carry

    lax.fori_loop(0, NZ, rotate, 0)
    pl.semaphore_wait(barrier, others + 3)

    def channels(ref, h):
        return ref.at[:, pl.ds(pl.multiple_of(h * HD, HD), HD)]

    def of_head(ref, h):
        return channels(ref, h) if ref is v or ref is c else ref.at[h]

    def arrived(ref, sem):
        pltpu.make_async_copy(ref, ref, sem).wait()

    def push(src, dst, s, r, peer):
        pltpu.make_async_remote_copy(src, dst, s, r, device_id=peer, device_id_type=MESH).start()

    own_a, own_b = z * LAYER + x, z * LAYER + LAYER - 1

    def rows(ref, start):
        return ref.at[pl.ds(pl.multiple_of(start, 8), TOK)]

    def rows_of(n):
        return n * SPAN + z * TOK

    def send_b(pairs):
        def run(n, carry):
            tz = lax.rem(z + n, NZ)
            h, peer = tz * LAYER + LAYER - 1, at_xz(x, tz)
            for s, src, r, dst in pairs:
                push(of_head(src, h), rows(dst, z * TOK), send.at[s], recv.at[r], peer)
            return carry
        for s, src, r, dst in pairs:
            pltpu.make_async_copy(of_head(src, own_b), rows(dst, z * TOK), recv.at[r]).start()
        lax.fori_loop(1, NZ, run, 0)

    def send_a(pairs, relative):
        def where(tx):
            return rows_of(lax.rem(x - tx + NX + NX - 1, NX)) if relative else rows_of(x)
        def run(n, carry):
            tx, tz = lax.rem(x + n // NZ, NX), lax.rem(z + lax.rem(n, NZ), NZ)
            h, peer = tz * LAYER + tx, at_xz(tx, tz)
            for s, src, r, dst in pairs:
                push(of_head(src, h), rows(dst, where(tx)), send.at[s], recv.at[r], peer)
            return carry
        for s, src, r, dst in pairs:
            pltpu.make_async_copy(of_head(src, own_a), rows(dst, where(x)), recv.at[r]).start()
        lax.fori_loop(1, NX * NZ, run, 0)

    send_b(((2, k, 0, kb_h), (3, v, 1, vb_h), (0, q, 2, qb_h)))
    def text_pieces(n):
        tx = lax.rem(x + n, NX)
        for ab, h in ((0, tx), (1, LAYER - 1)):
            for t, src in enumerate((text_key, text_value)):
                yield channels(src, h), txt.at[zl, y, x, ab, t], {"blk_0": tx, "blk_2": core, "uly_1": zl}

    for n in range(1, NX):
        for src, dst, peer in text_pieces(n):
            push(src, dst, text_send.at[0], text_recv.at[0], peer)

    @pl.when(zl != core)
    def _():
        for src, dst, peer in text_pieces(0):
            push(src, dst, text_send.at[3], text_recv.at[0], peer)

    @pl.when(zl == core)
    def _():
        for src, dst, peer in text_pieces(0):
            pltpu.make_async_copy(src, dst, text_recv.at[0]).start()

    send_a(((2, k, 3, ka_h),), False)
    send_a(((3, v, 4, va_h),), False)
    send_a(((0, q, 5, qa_h),), True)
    send_b(((1, c, 6, cb_h),))
    send_a(((1, c, 7, ca_h),), True)

    qb[:, SPAN:, :] = jnp.zeros((NX, WIDE - SPAN, HD), jnp.bfloat16)
    cb[SPAN:, :] = jnp.zeros((WIDE - SPAN, HD), jnp.bfloat16)
    row_m[...] = jnp.full_like(row_m, NEG)
    row_l[...] = jnp.zeros_like(row_l)
    acc[...] = jnp.zeros_like(acc)
    stat[...] = jnp.zeros_like(stat)

    def give(kind, region, target, n, which=(0, 1)):
        for t in which:
            push(region(kind[t]), region(kind[t]), ring_send.at[n, t], ring_recv.at[n, t], {"blk_1": target})

    def took(kind, region, n, which=(0, 1)):
        for t in which:
            arrived(region(kind[t]), ring_recv.at[n, t])

    def share(kind, region, n, which=(0, 1)):
        for t in which:
            push(region(kind[t]), region(kind[t]), twin_send.at[n, t], twin_recv.at[n, t], twin)

    def land(src, dst, r, n):
        arrived(src, recv.at[r])
        pltpu.make_async_copy(src, dst, local.at[n]).start()
        return lambda: pltpu.make_async_copy(src, dst, local.at[n]).wait()

    a, b = (ka, va), (kb, vb)
    mine = core * NY
    a_y = lambda yy: lambda r: r.at[mine + yy]
    a_half = lambda yy, s: lambda r: r.at[mine + yy, pl.ds(s * (REGION // 2), REGION // 2)]
    b_y = lambda yy: lambda r: r.at[core, yy]
    b_half = lambda yy, s: lambda r: r.at[core, yy, pl.ds(s * (SPAN // 2), SPAN // 2)]
    b_all = lambda r: r.at[core]

    for done in [land(kb_h, kb.at[core, y], 0, 0), land(vb_h, vb.at[core, y], 1, 1)]:
        done()
    give(b, b_y(y), yp, 0)
    give(b, b_y(y), ym, 1)
    land(qb_h, qb.at[0, pl.ds(0, SPAN)], 2, 2)()
    for n in range(1, NX):
        push(qb.at[0, pl.ds(0, SPAN)], qb.at[NX - n, pl.ds(0, SPAN)], fan_send.at[n - 1], fan_recv.at[NX - n - 1],
             {"blk_0": lax.rem(x + n, NX)})
    arrived(txt.at[core, y], text_recv.at[0])
    for yy in (yp, ym, yo):
        push(txt.at[core, y], txt.at[core, y], text_send.at[1], text_recv.at[1], {"blk_1": yy})
    took(b, b_y(ym), 0)
    give(b, b_half(ym, 0), yp, 2)
    took(b, b_y(yp), 1)
    give(b, b_half(yp, 1), ym, 3)
    took(b, b_half(yo, 0), 2)
    took(b, b_half(yo, 1), 3)
    share(b, b_all, 4)
    arrived(txt.at[core, pl.ds(0, NY - 1)], text_recv.at[1])
    push(txt.at[core], txt.at[core], text_send.at[2], text_recv.at[2], twin)
    for n in range(1, NX):
        arrived(qb.at[n, pl.ds(0, SPAN)], fan_recv.at[n - 1])

    held = (s0, s1)

    def absorb(cols, width, s, peak, values):
        m = row_m[0:1, cols]
        new = jnp.maximum(m, peak)
        shrink = jnp.exp2((m - new) * SCALE)
        p = jnp.exp2((s[:, :width] - new) * SCALE)
        row_m[0:1, cols] = new
        row_l[0:1, cols] = row_l[0:1, cols] * shrink + jnp.sum(p, axis=0, keepdims=True)
        acc[:, cols] = acc[:, cols] * shrink + jnp.dot(
            values[...], p.astype(jnp.bfloat16), preferred_element_type=jnp.float32)

    def attend(queries, width, scores):
        peaks = scores(queries[0][0], s0)
        for n, (_, cols) in enumerate(queries):
            ahead = scores(queries[n + 1][0], held[(n + 1) % 2]) if n + 1 < len(queries) else None
            absorb(cols, width, held[n % 2], peaks, vt)
            peaks = ahead

    limit = KEYS - (NX - 1) * LAST - pad_ref[0]
    limit_b = jnp.where(x == NX - 1, limit, LAST)

    def masked(s, cc, yy, bound):
        cells = jnp.concatenate([place_in_frame[...]] * (s.shape[1] // HD), axis=1)
        return jnp.where(cells < bound - yy * (2 * TH * GRID_W) - cc * TW, s, NEG)

    def own_region(t):
        land((ka_h, va_h)[t], a[t].at[mine + y], 3 + t, 3 + t)()
        give(a, a_y(y), yp, 4, (t,))
        give(a, a_y(y), ym, 5, (t,))
        share(a, a_y(y), 0, (t,))

    def pass_on(t):
        took(a, a_y(ym), 4, (t,))
        give(a, a_half(ym, 0), yp, 6, (t,))
        share(a, a_y(ym), 1, (t,))
        took(a, a_y(yp), 5, (t,))
        give(a, a_half(yp, 1), ym, 7, (t,))
        share(a, a_y(yp), 2, (t,))

    b_tiles = [(n, slice(n * WIDE, (n + 1) * WIDE)) for n in range(NX)]

    def b_region(i, carry):
        cc = lax.rem(core + i, NC)

        @pl.when(i == 1)
        def _():
            for t in range(2):
                arrived(b[t].at[1 - core], twin_recv.at[4, t])

        vt[...] = vb[cc].reshape(REGION, HD).T

        def scores(n, into):
            s = lax.dot_general(kb[cc].reshape(REGION, HD), qb[n], NT, preferred_element_type=jnp.float32)
            peak = jnp.full((1, WIDE), NEG, jnp.float32)
            for yy in range(NY):
                cut = slice(yy * SPAN, (yy + 1) * SPAN)
                e = masked(s[cut], cc, yy, limit_b)
                into[cut, :] = e
                peak = jnp.maximum(peak, jnp.max(e, axis=0, keepdims=True))
            return peak

        attend(b_tiles, WIDE, scores)
        return carry

    own_region(0)
    lax.fori_loop(0, NC, b_region, 0)
    for n in range(NX):
        cols = slice(n * WIDE, (n + 1) * WIDE)
        part[n] = (acc[:, cols] / row_l[0:1, cols]).astype(jnp.bfloat16)
        stat[n, 0:1, :] = row_m[0:1, cols]
        stat[n, 1:2, :] = row_l[0:1, cols]
    for n in range(1, NX):
        peer = {"blk_0": lax.rem(x + n, NX)}
        push(part.at[n], part.at[NX + n], part_send.at[n - 1, 0], part_recv.at[n - 1, 0], peer)
        push(stat.at[n], stat.at[NX + n], part_send.at[n - 1, 1], part_recv.at[n - 1, 1], peer)

    row_m[...] = jnp.full_like(row_m, NEG)
    row_l[...] = jnp.zeros_like(row_l)
    acc[...] = jnp.zeros_like(acc)

    own_region(1)
    pass_on(0)

    def ordered(cols):
        return lax.dot_general(perm[...], cols, NT, preferred_element_type=jnp.float32).reshape(
            GROUPS, PAD, HD)[:, :PIECE].astype(jnp.bfloat16)

    def landing(result, head):
        return result.at[core, :, pl.ds(pl.multiple_of(head * HD, HD), HD)]

    def deliver(src, result, n, head, which):
        for m in range(1 if n == 0 else 0, GROUPS):
            g, peer = owner(n, m)
            push(src.at[g], landing(result, head), out_send.at[which], out_recv.at[which], peer)

    def keep(src, result, head, n):
        return pltpu.make_async_copy(src.at[zl * 8 + core * 4 + zh], landing(result, head), near.at[n])

    a_tiles = [(slice(n * TILE, (n + 1) * TILE),) * 2 for n in range(REGION // TILE)]

    def text_rows(ab, kv):
        return txt[:, :, :, ab, kv].reshape(-1, HD)

    def text_scores(q_tile, keys, into):
        s = lax.dot_general(keys, q_tile, NT, preferred_element_type=jnp.float32)
        into[:TEXT, : q_tile.shape[0]] = s
        return jnp.max(s, axis=0, keepdims=True)

    def text_mix(s, width, peak, values_t):
        p = jnp.exp2((s[:TEXT, :width] - peak) * SCALE)
        weighted = jnp.dot(values_t, p.astype(jnp.bfloat16), preferred_element_type=jnp.float32)
        return (weighted / jnp.sum(p, axis=0, keepdims=True)).astype(jnp.bfloat16)

    def merge_parts():
        for n in range(1, NX):
            arrived(part.at[NX + n], part_recv.at[n - 1, 0])
            arrived(stat.at[NX + n], part_recv.at[n - 1, 1])
        slots = [0] + [NX + n for n in range(1, NX)]
        top = stat[0, 0:1, :]
        for n in slots[1:]:
            top = jnp.maximum(top, stat[n, 0:1, :])
        weights = [stat[n, 1:2, :] * jnp.exp2((stat[n, 0:1, :] - top) * SCALE) for n in slots]
        total = weights[0] + weights[1] + weights[2] + weights[3]
        merged = part[0].astype(jnp.float32) * (weights[0] / total)
        for n, w in zip(slots[1:], weights[1:]):
            merged = merged + part[n].astype(jnp.float32) * (w / total)
        ob[...] = ordered(merged.astype(jnp.bfloat16)[:, :SPAN])
        keep(ob, rs, own_b, 0).start()
        deliver(ob, rs, 0, own_b, 0)

    def attend_text():
        arrived(txt.at[1 - core], text_recv.at[2])
        land(cb_h, cb.at[pl.ds(0, SPAN)], 6, 6)()
        land(ca_h, ca, 7, 7)()
        keys_b, values_b = text_rows(1, 0), text_rows(1, 1).T
        keys, values_t = text_rows(0, 0), text_rows(0, 1).T
        peak_b = text_scores(cb[...], keys_b, s0)
        peak = text_scores(ca[a_tiles[0][0], :], keys, s1)
        result_b = text_mix(s0, WIDE, peak_b, values_b)
        for n, (cols, _) in enumerate(a_tiles):
            if n + 1 < len(a_tiles):
                ahead = text_scores(ca[a_tiles[n + 1][0], :], keys, held[n % 2])
            ot[:, cols] = text_mix(held[(n + 1) % 2], TILE, peak, values_t)
            peak = ahead
            if n > 0:
                oc[n - 1] = ordered(ot[:, (n - 1) * SPAN : n * SPAN])
                deliver(oc.at[n - 1], rc, n % NX, own_a, 1)
        keep(oc.at[NX - 1], rc, own_a, 2).start()
        od[...] = ordered(result_b[:, :SPAN])
        keep(od, rc, own_b, 1).start()
        deliver(od, rc, 0, own_b, 1)

    def region_of(i):
        theirs = jnp.logical_or(i == 1, jnp.logical_or(jnp.logical_or(i == 4, i == 5), i == 7))
        cc = jnp.where(theirs, 1 - core, core)
        yy = jnp.where(i < 2, y, jnp.where(i >= 6, yo, jnp.where(lax.rem(i, 2) == 0, ym, yp)))
        return cc, yy, cc * NY + yy

    def a_scores(region, cols, into):
        cc, yy, at = region
        q_tile = qa[cols, :]
        s = lax.dot_general(ka[at, : REGION - SPAN, :], q_tile, NT, preferred_element_type=jnp.float32)
        into[: REGION - SPAN, :TILE] = s
        e = lax.dot_general(ka[at, REGION - SPAN :, :], q_tile, NT, preferred_element_type=jnp.float32)
        e = masked(e, cc, yy, limit)
        into[REGION - SPAN :, :TILE] = e
        return jnp.maximum(jnp.max(s, axis=0, keepdims=True), jnp.max(e, axis=0, keepdims=True))

    def a_region(i, carry):
        region = region_of(i)

        @pl.when(i == 1)
        def _():
            for t in range(2):
                arrived(a[t].at[region[2]], twin_recv.at[0, t])

        @pl.when(i == 2)
        def _():
            pass_on(1)
            merge_parts()

        @pl.when(i == 3)
        def _():
            attend_text()

        vt[...] = va[region[2]].T
        attend(a_tiles, TILE, lambda cols, into: a_scores(region, cols, into))
        return carry

    land(qa_h, qa, 5, 5)()
    lax.fori_loop(0, 4, a_region, 0)
    took(a, a_half(yo, 0), 6)
    took(a, a_half(yo, 1), 7)
    share(a, a_y(yo), 3)

    last = [region_of(i) for i in (4, 5, 6, 7)]
    for (cc, yy, at), n in ((last[0], 1), (last[1], 2), (last[3], 3)):
        for t in range(2):
            arrived(a[t].at[at], twin_recv.at[n, t])
    for n, region in enumerate(last):
        vt4[n] = va[region[2]].T

    def a_tile(t, peak):
        cols = pl.ds(pl.multiple_of(t * TILE, TILE), TILE)
        after = pl.ds(pl.multiple_of(jnp.minimum(t + 1, REGION // TILE - 1) * TILE, TILE), TILE)
        for n in range(4):
            if n < 3:
                ahead = a_scores(last[n + 1], cols, held[(n + 1) % 2])
            else:
                ahead = a_scores(last[0], after, held[0])
            absorb(cols, TILE, held[n % 2], peak, vt4.at[n])
            peak = ahead
        ot[:, cols] = (acc[:, cols] / row_l[0:1, cols]).astype(jnp.bfloat16)
        for n in range(NX):
            @pl.when(t == n + 1)
            def _():
                oa[n] = ordered(ot[:, n * SPAN : (n + 1) * SPAN])
                if n == NX - 1:
                    keep(oa.at[n], rs, own_a, 3).start()
                deliver(oa.at[n], rs, (n + 1) % NX, own_a, 0)
        return peak

    lax.fori_loop(0, REGION // TILE, a_tile, a_scores(last[0], slice(0, TILE), held[0]))

    for n in range(4):
        arrived(v.at[:, pl.ds(0, (NX * NZ - 1 + NZ - 1) * HD)], send.at[n])
    for t in range(2):
        for n in (0, 1):
            arrived(b_y(y)(b[t]), ring_send.at[n, t])
            arrived(b_half(y, 0)(b[t]), ring_send.at[2 + n, t])
            arrived(a_y(y)(a[t]), ring_send.at[4 + n, t])
            arrived(a_half(y, 0)(a[t]), ring_send.at[6 + n, t])
        for n in range(4):
            arrived(a_y(y)(a[t]), twin_send.at[n, t])
        arrived(b[t].at[core], twin_send.at[4, t])
    for n in range(1, NX):
        arrived(qb.at[n, pl.ds(0, SPAN)], fan_send.at[n - 1])
        arrived(part.at[n], part_send.at[n - 1, 0])
        arrived(stat.at[n], part_send.at[n - 1, 1])
    arrived(txt.at[core, y, pl.ds(0, NX - 1)], text_send.at[0])

    @pl.when(zl != core)
    def _():
        arrived(txt.at[core, y, 0], text_send.at[3])

    arrived(txt.at[core, pl.ds(0, NY - 1)], text_send.at[1])
    arrived(txt.at[core], text_send.at[2])
    keep(ob, rs, own_b, 0).wait()
    keep(od, rc, own_b, 1).wait()
    keep(oc.at[NX - 1], rc, own_a, 2).wait()
    keep(oa.at[NX - 1], rs, own_a, 3).wait()
    for n, r, out in ((1, rc, out_c), (0, rs, out_s)):
        moved = r.at[:, :, pl.ds(0, (others + NZ * NC - 1) // 2 * HD)]
        arrived(moved, out_recv.at[n])
        out[...] = sum(jnp.dot(rows_to_own(cc), r[cc], preferred_element_type=jnp.float32)
                       for cc in range(NC)).astype(jnp.bfloat16)
        arrived(moved, out_send.at[n])


def rows_to_own(core):
    to = lax.broadcasted_iota(jnp.int32, (TOK, PIECE), 0)
    piece = lax.broadcasted_iota(jnp.int32, (TOK, PIECE), 1)
    return jnp.where(to == piece + (piece // TW) * TW + core * TW, 1.0, 0.0).astype(jnp.bfloat16)


def block(pad, q, k, v, c, text_key, text_value):
    any_spec = pl.BlockSpec(memory_space=pl.ANY)
    vmem = pl.BlockSpec(memory_space=pltpu.VMEM)
    dma = pltpu.SemaphoreType.DMA
    half = lambda *s: pltpu.VMEM(s, jnp.bfloat16)
    full = lambda *s: pltpu.VMEM(s, jnp.float32)
    landing = [REGION, REGION, SPAN, SPAN, REGION, REGION, SPAN, SPAN]
    result = jax.ShapeDtypeStruct((TOK, HEADS * HD), jnp.bfloat16)
    return pl.pallas_call(
        block_kernel,
        in_specs=[any_spec] * 8,
        out_specs=[vmem] * 2 + [any_spec] * 8,
        out_shape=[result] * 2 + [jax.ShapeDtypeStruct((n, HD), jnp.bfloat16) for n in landing],
        scratch_shapes=[
            pltpu.SMEM((1,), jnp.int32), full(8, HD), half(GROUPS * PAD, SPAN), pltpu.VMEM((SPAN, HD), jnp.int32),
            half(NC, PIECE, HEADS * HD), half(NC, PIECE, HEADS * HD),
            half(TOK, HEADS * HD), half(TOK, HEADS * HD), half(HEADS, TOK, HD), half(HEADS, TOK, HD),
            half(REGION, HD), half(NX, WIDE, HD), half(REGION, HD), half(WIDE, HD),
            half(NC * NY, REGION, HD), half(NC * NY, REGION, HD), half(NC, NY, SPAN, HD), half(NC, NY, SPAN, HD),
            half(NC, NY, NX, 2, 2, 16, HD),
            full(REGION, WIDE), full(REGION, WIDE), half(HD, REGION), half(4, HD, REGION), full(HD, NX * WIDE),
            full(8, NX * WIDE), full(8, NX * WIDE), half(HD, REGION),
            half(NX, GROUPS, PIECE, HD), half(GROUPS, PIECE, HD), half(NX, GROUPS, PIECE, HD), half(GROUPS, PIECE, HD),
            half(2 * NX, HD, WIDE), full(2 * NX, 8, WIDE),
            dma((4,)), dma((8,)), dma((12,)), dma((8, 2)), dma((8, 2)), dma((5, 2)), dma((5, 2)), dma((3,)), dma((3,)),
            dma((3, 2)), dma((3, 2)), dma((4,)), dma((3,)), dma((2,)), dma((2,)), dma((4,)),
        ],
        compiler_params=pltpu.CompilerParams(collective_id=0, has_side_effects=True),
        name="block",
    )(pad, omega_table(), q, k, v, c, text_key, text_value)[:2]


def omega_table():
    pair = np.arange(HD) // 2
    side = HD // 6
    first = HD // 2 - 2 * side
    table = np.zeros((8, HD), np.float32)
    for axis, start, count in ((0, 0, first), (1, first, side), (2, first + side, side)):
        inside = (pair >= start) & (pair < start + count)
        table[axis] = np.where(inside, 10000.0 ** (-((pair - start) / count)), 0.0)
    table[3] = np.where(np.arange(HD) % 2 == 0, -1.0, 1.0)
    return jnp.asarray(table)


def body(self_query, self_key, self_value, cross_query, text_key, text_value, padded_count):
    return tuple(block(padded_count, self_query, self_key, self_value, cross_query, text_key, text_value))


def solution(mesh):
    split = Mesh(mesh.devices.reshape(4, 4, 2, 4, 2), BLK + ULY)
    own = P(BLK + ULY, None)
    return jax.shard_map(body, mesh=split, in_specs=(own,) * 4 + (P(BLK, ULY),) * 2 + (P(),),
                         out_specs=(own, own), check_vma=False)
```

```python
import functools
import math

import jax
import jax.numpy as jnp
import numpy as np
from jax import lax
from jax.experimental import pallas as pl
from jax.experimental.pallas import tpu as pltpu
from jax.sharding import Mesh
from jax.sharding import PartitionSpec as P

HD = 128
TH = 4
TW = 10
TOK = TH * TW
ROW_TILES = 8
NX, NY, NZ, NC = 4, 4, 8, 2
LAYER = 5
HEADS = NZ * LAYER
GRID_H = TH * ROW_TILES
GRID_W = TW * NZ
KEYS = NX * NY * NZ * NC * TOK
TEXT = 512
LAST = KEYS // NX
PIECE = 2 * TW
PAD = 24
GROUPS = 16
ULY = ("uly_0", "uly_1")
BLK = ("blk_0", "blk_1", "blk_2")
NEG = -1e30
MESH = pl.DeviceIdType.MESH


def place():
    x = lax.axis_index("blk_0")
    y = lax.axis_index("blk_1")
    z = lax.axis_index("uly_0") * 2 + lax.axis_index("blk_2")
    return x, y, z, lax.axis_index("uly_1")


def at_xz(x, z):
    return {"blk_0": x, "uly_0": z // 2, "blk_2": lax.rem(z, 2)}


SPAN = NZ * TOK
REGION = NX * SPAN
WIDE = 384
TILE = 256
SCALE = math.log2(math.e) / math.sqrt(HD)
NT = (((1,), (1,)), ((), ()))


def block_kernel(
    pad_hbm, omegas_hbm, q_hbm, k_hbm, v, c, text_key, text_value,
    out_s, out_c, qa_h, ca_h, qb_h, cb_h, ka_h, va_h, kb_h, vb_h,
    pad_ref, omegas, perm, place_in_frame, rs, rc, q_in, k_in, q, k, qa, qb, ca, cb, ka, va, kb, vb, txt, s0, s1, vt, vt4, acc, row_m, row_l, ot, oa, ob, oc, od, part, stat,
    send, recv, local, ring_send, ring_recv, twin_send, twin_recv, fan_send, fan_recv, part_send, part_recv,
    text_send, text_recv, out_send, out_recv, near,
):
    x, y, z, core = place()
    zl, zh = lax.axis_index("blk_2"), lax.axis_index("uly_0")
    twin = {"uly_1": 1 - core}
    yp, ym, yo = lax.rem(y + 1, NY), lax.rem(y + NY - 1, NY), lax.rem(y + 2, NY)
    others = NX * NZ * NC - 1

    def owner(n, m):
        ti = lax.rem(zh + m // 4, 4)
        tl = lax.rem(zl + lax.rem(m // 2, 2), 2)
        ta = lax.rem(core + lax.rem(m, 2), 2)
        peer = {"blk_0": lax.rem(x + n, NX), "uly_0": ti, "blk_2": tl, "uly_1": ta}
        return tl * 8 + ta * 4 + ti, peer

    loads = [pltpu.make_async_copy(src, dst, local.at[8 + n]) for n, (src, dst) in enumerate(
        ((k_hbm, k_in), (q_hbm, q_in), (omegas_hbm, omegas), (pad_hbm, pad_ref)))]
    for load in loads:
        load.start()
    barrier = pltpu.get_barrier_semaphore()

    for n in (2, 1, 3, 0):
        for zz in (2, 1, 3, 0):
            for m in range(4):
                if (n, zz, m) != (0, 0, 0):
                    peer = owner(n, zz * 4 + m)[1]
                    pl.semaphore_signal(barrier, inc=1, device_id=peer, device_id_type=MESH)
    for yy in (yp, ym, yo):
        pl.semaphore_signal(barrier, inc=1, device_id={"blk_1": yy}, device_id_type=MESH)

    n = lax.broadcasted_iota(jnp.int32, (SPAN, HD), 0)
    n_z, n_t = n // TOK, lax.rem(n, TOK)
    place_in_frame[...] = (lax.rem(n_z, 2) * TH + n_t // TW) * GRID_W + (n_z // 2) * (2 * TW) + lax.rem(n_t, TW)
    to = lax.broadcasted_iota(jnp.int32, (GROUPS * PAD, SPAN), 0)
    at = lax.broadcasted_iota(jnp.int32, (GROUPS * PAD, SPAN), 1)
    g, r = to // PAD, lax.rem(to, PAD)
    wanted = ((2 * (2 * (lax.rem(g, 8) // TH) + r // TW) + g // 8) * TOK + lax.rem(g, TH) * TW + lax.rem(r, TW))
    perm[...] = jnp.where(jnp.logical_and(at == wanted, r < PIECE), 1.0, 0.0).astype(jnp.bfloat16)

    for load in loads:
        load.wait()
    token = lax.broadcasted_iota(jnp.int32, (TOK, HD), 0)
    chunk = (x * NY + y) * 2 + zl
    row = lax.rem(chunk, ROW_TILES) * TH + token // TW
    col = (zh * 2 + core) * TW + lax.rem(token, TW)
    angles = (jnp.full((TOK, HD), chunk // ROW_TILES).astype(jnp.float32) * omegas[0:1, :]
              + row.astype(jnp.float32) * omegas[1:2, :] + col.astype(jnp.float32) * omegas[2:3, :])
    cos, sin = jnp.cos(angles), jnp.sin(angles) * omegas[3:4, :]
    even = lax.rem(lax.broadcasted_iota(jnp.int32, (TOK, HD), 1), 2) == 0

    def rotate(n, carry):
        for src, dst in ((k_in, k), (q_in, q)):
            for h in range(LAYER):
                wide = src[:, pl.ds(pl.multiple_of((n * LAYER + h) * HD, HD), HD)].astype(jnp.float32)
                partner = jnp.where(even, pltpu.roll(wide, HD - 1, 1), pltpu.roll(wide, 1, 1))
                dst[n * LAYER + h] = (wide * cos + partner * sin).astype(jnp.bfloat16)
        return carry

    lax.fori_loop(0, NZ, rotate, 0)
    pl.semaphore_wait(barrier, others + 3)

    def channels(ref, h):
        return ref.at[:, pl.ds(pl.multiple_of(h * HD, HD), HD)]

    def of_head(ref, h):
        return channels(ref, h) if ref is v or ref is c else ref.at[h]

    def arrived(ref, sem):
        pltpu.make_async_copy(ref, ref, sem).wait()

    def push(src, dst, s, r, peer):
        pltpu.make_async_remote_copy(src, dst, s, r, device_id=peer, device_id_type=MESH).start()

    own_a, own_b = z * LAYER + x, z * LAYER + LAYER - 1

    def rows(ref, start):
        return ref.at[pl.ds(pl.multiple_of(start, 8), TOK)]

    def rows_of(n):
        return n * SPAN + z * TOK

    def z_offset(n):
        return lax.rem(jnp.where(lax.rem(n, 2) == 1, 4 + (n + 1) // 2, 4 - n // 2), NZ)

    def x_offset(n):
        return jnp.where(n < 2, 2 - n, jnp.where(n == 2, 3, 0))

    def send_b(pairs):
        def run(n, carry):
            tz = lax.rem(z + z_offset(n), NZ)
            h, peer = tz * LAYER + LAYER - 1, at_xz(x, tz)
            for s, src, r, dst in pairs:
                push(of_head(src, h), rows(dst, z * TOK), send.at[s], recv.at[r], peer)
            return carry
        for s, src, r, dst in pairs:
            pltpu.make_async_copy(of_head(src, own_b), rows(dst, z * TOK), recv.at[r]).start()
        lax.fori_loop(0, NZ - 1, run, 0)

    def send_a(pairs, relative):
        def where(tx):
            return rows_of(lax.rem(x - tx + NX + NX - 1, NX)) if relative else rows_of(x)
        def run(n, carry):
            tx, tz = lax.rem(x + x_offset(n // NZ), NX), lax.rem(z + z_offset(lax.rem(n, NZ)), NZ)
            h, peer = tz * LAYER + tx, at_xz(tx, tz)
            for s, src, r, dst in pairs:
                push(of_head(src, h), rows(dst, where(tx)), send.at[s], recv.at[r], peer)
            return carry
        for s, src, r, dst in pairs:
            pltpu.make_async_copy(of_head(src, own_a), rows(dst, where(x)), recv.at[r]).start()
        lax.fori_loop(0, NX * NZ - 1, run, 0)

    send_b(((2, k, 0, kb_h), (3, v, 1, vb_h), (0, q, 2, qb_h)))
    def text_pieces(n):
        tx = lax.rem(x + n, NX)
        for ab, h in ((0, tx), (1, LAYER - 1)):
            for t, src in enumerate((text_key, text_value)):
                yield channels(src, h), txt.at[zl, y, x, ab, t], {"blk_0": tx, "blk_2": core, "uly_1": zl}

    for n in range(1, NX):
        for src, dst, peer in text_pieces(n):
            push(src, dst, text_send.at[0], text_recv.at[0], peer)

    @pl.when(zl != core)
    def _():
        for src, dst, peer in text_pieces(0):
            push(src, dst, text_send.at[3], text_recv.at[0], peer)

    @pl.when(zl == core)
    def _():
        for src, dst, peer in text_pieces(0):
            pltpu.make_async_copy(src, dst, text_recv.at[0]).start()

    send_a(((2, k, 3, ka_h),), False)
    send_a(((3, v, 4, va_h),), False)
    send_a(((0, q, 5, qa_h),), True)
    send_b(((1, c, 6, cb_h),))
    send_a(((1, c, 7, ca_h),), True)

    qb[:, SPAN:, :] = jnp.zeros((NX, WIDE - SPAN, HD), jnp.bfloat16)
    cb[SPAN:, :] = jnp.zeros((WIDE - SPAN, HD), jnp.bfloat16)
    row_m[...] = jnp.full_like(row_m, NEG)
    row_l[...] = jnp.zeros_like(row_l)
    acc[...] = jnp.zeros_like(acc)
    stat[...] = jnp.zeros_like(stat)

    def give(kind, region, target, n, which=(0, 1)):
        for t in which:
            push(region(kind[t]), region(kind[t]), ring_send.at[n, t], ring_recv.at[n, t], {"blk_1": target})

    def took(kind, region, n, which=(0, 1)):
        for t in which:
            arrived(region(kind[t]), ring_recv.at[n, t])

    def share(kind, region, n, which=(0, 1)):
        for t in which:
            push(region(kind[t]), region(kind[t]), twin_send.at[n, t], twin_recv.at[n, t], twin)

    def land(src, dst, r, n):
        arrived(src, recv.at[r])
        pltpu.make_async_copy(src, dst, local.at[n]).start()
        return lambda: pltpu.make_async_copy(src, dst, local.at[n]).wait()

    a, b = (ka, va), (kb, vb)
    mine = core * NY
    a_y = lambda yy: lambda r: r.at[mine + yy]
    a_half = lambda yy, s: lambda r: r.at[mine + yy, pl.ds(s * (REGION // 2), REGION // 2)]
    b_y = lambda yy: lambda r: r.at[core, yy]
    b_half = lambda yy, s: lambda r: r.at[core, yy, pl.ds(s * (SPAN // 2), SPAN // 2)]
    b_all = lambda r: r.at[core]

    for done in [land(kb_h, kb.at[core, y], 0, 0), land(vb_h, vb.at[core, y], 1, 1)]:
        done()
    give(b, b_y(y), yp, 0)
    give(b, b_y(y), ym, 1)
    land(qb_h, qb.at[0, pl.ds(0, SPAN)], 2, 2)()
    for n in range(1, NX):
        push(qb.at[0, pl.ds(0, SPAN)], qb.at[NX - n, pl.ds(0, SPAN)], fan_send.at[n - 1], fan_recv.at[NX - n - 1],
             {"blk_0": lax.rem(x + n, NX)})
    arrived(txt.at[core, y], text_recv.at[0])
    for yy in (yp, ym, yo):
        push(txt.at[core, y], txt.at[core, y], text_send.at[1], text_recv.at[1], {"blk_1": yy})
    took(b, b_y(ym), 0)
    give(b, b_half(ym, 0), yp, 2)
    took(b, b_y(yp), 1)
    give(b, b_half(yp, 1), ym, 3)
    took(b, b_half(yo, 0), 2)
    took(b, b_half(yo, 1), 3)
    share(b, b_all, 4)
    arrived(txt.at[core, pl.ds(0, NY - 1)], text_recv.at[1])
    push(txt.at[core], txt.at[core], text_send.at[2], text_recv.at[2], twin)
    for n in range(1, NX):
        arrived(qb.at[n, pl.ds(0, SPAN)], fan_recv.at[n - 1])

    held = (s0, s1)

    def absorb(cols, width, s, peak, values):
        m = row_m[0:1, cols]
        new = jnp.maximum(m, peak)
        shrink = jnp.exp2((m - new) * SCALE)
        p = jnp.exp2((s[:, :width] - new) * SCALE)
        row_m[0:1, cols] = new
        row_l[0:1, cols] = row_l[0:1, cols] * shrink + jnp.sum(p, axis=0, keepdims=True)
        acc[:, cols] = acc[:, cols] * shrink + jnp.dot(
            values[...], p.astype(jnp.bfloat16), preferred_element_type=jnp.float32)

    def attend(queries, width, scores):
        peaks = scores(queries[0][0], s0)
        for n, (_, cols) in enumerate(queries):
            ahead = scores(queries[n + 1][0], held[(n + 1) % 2]) if n + 1 < len(queries) else None
            absorb(cols, width, held[n % 2], peaks, vt)
            peaks = ahead

    limit = KEYS - (NX - 1) * LAST - pad_ref[0]
    limit_b = jnp.where(x == NX - 1, limit, LAST)

    def masked(s, cc, yy, bound):
        cells = jnp.concatenate([place_in_frame[...]] * (s.shape[1] // HD), axis=1)
        return jnp.where(cells < bound - yy * (2 * TH * GRID_W) - cc * TW, s, NEG)

    def own_region(t):
        land((ka_h, va_h)[t], a[t].at[mine + y], 3 + t, 3 + t)()
        give(a, a_y(y), yp, 4, (t,))
        give(a, a_y(y), ym, 5, (t,))
        share(a, a_y(y), 0, (t,))

    def pass_on(t):
        took(a, a_y(ym), 4, (t,))
        give(a, a_half(ym, 0), yp, 6, (t,))
        share(a, a_y(ym), 1, (t,))
        took(a, a_y(yp), 5, (t,))
        give(a, a_half(yp, 1), ym, 7, (t,))
        share(a, a_y(yp), 2, (t,))

    b_tiles = [(n, slice(n * WIDE, (n + 1) * WIDE)) for n in range(NX)]

    def b_region(i, carry):
        cc = lax.rem(core + i, NC)

        @pl.when(i == 1)
        def _():
            for t in range(2):
                arrived(b[t].at[1 - core], twin_recv.at[4, t])

        vt[...] = vb[cc].reshape(REGION, HD).T

        def scores(n, into):
            s = lax.dot_general(kb[cc].reshape(REGION, HD), qb[n], NT, preferred_element_type=jnp.float32)
            peak = jnp.full((1, WIDE), NEG, jnp.float32)
            for yy in range(NY):
                cut = slice(yy * SPAN, (yy + 1) * SPAN)
                e = masked(s[cut], cc, yy, limit_b)
                into[cut, :] = e
                peak = jnp.maximum(peak, jnp.max(e, axis=0, keepdims=True))
            return peak

        attend(b_tiles, WIDE, scores)
        return carry

    own_region(0)
    lax.fori_loop(0, NC, b_region, 0)
    for n in range(NX):
        cols = slice(n * WIDE, (n + 1) * WIDE)
        part[n] = (acc[:, cols] / row_l[0:1, cols]).astype(jnp.bfloat16)
        stat[n, 0:1, :] = row_m[0:1, cols]
        stat[n, 1:2, :] = row_l[0:1, cols]
    for n in range(1, NX):
        peer = {"blk_0": lax.rem(x + n, NX)}
        push(part.at[n], part.at[NX + n], part_send.at[n - 1, 0], part_recv.at[n - 1, 0], peer)
        push(stat.at[n], stat.at[NX + n], part_send.at[n - 1, 1], part_recv.at[n - 1, 1], peer)

    row_m[...] = jnp.full_like(row_m, NEG)
    row_l[...] = jnp.zeros_like(row_l)
    acc[...] = jnp.zeros_like(acc)

    own_region(1)
    pass_on(0)

    def ordered(cols):
        return lax.dot_general(perm[...], cols, NT, preferred_element_type=jnp.float32).reshape(
            GROUPS, PAD, HD)[:, :PIECE].astype(jnp.bfloat16)

    def landing(result, head):
        return result.at[core, :, pl.ds(pl.multiple_of(head * HD, HD), HD)]

    def deliver(src, result, n, head, which):
        for m in (8, 9, 10, 11, 4, 5, 6, 7, 12, 13, 14, 15, 2, 3, 1) + ((0,) if n else ()):
            g, peer = owner(n, m)
            push(src.at[g], landing(result, head), out_send.at[which], out_recv.at[which], peer)

    def keep(src, result, head, n):
        return pltpu.make_async_copy(src.at[zl * 8 + core * 4 + zh], landing(result, head), near.at[n])

    a_tiles = [(slice(n * TILE, (n + 1) * TILE),) * 2 for n in range(REGION // TILE)]

    def text_rows(ab, kv):
        return txt[:, :, :, ab, kv].reshape(-1, HD)

    def text_scores(q_tile, keys, into):
        s = lax.dot_general(keys, q_tile, NT, preferred_element_type=jnp.float32)
        into[:TEXT, : q_tile.shape[0]] = s
        return jnp.max(s, axis=0, keepdims=True)

    def text_mix(s, width, peak, values_t):
        p = jnp.exp2((s[:TEXT, :width] - peak) * SCALE)
        weighted = jnp.dot(values_t, p.astype(jnp.bfloat16), preferred_element_type=jnp.float32)
        return (weighted / jnp.sum(p, axis=0, keepdims=True)).astype(jnp.bfloat16)

    def merge_parts():
        for n in range(1, NX):
            arrived(part.at[NX + n], part_recv.at[n - 1, 0])
            arrived(stat.at[NX + n], part_recv.at[n - 1, 1])
        slots = [0] + [NX + n for n in range(1, NX)]
        top = stat[0, 0:1, :]
        for n in slots[1:]:
            top = jnp.maximum(top, stat[n, 0:1, :])
        weights = [stat[n, 1:2, :] * jnp.exp2((stat[n, 0:1, :] - top) * SCALE) for n in slots]
        total = weights[0] + weights[1] + weights[2] + weights[3]
        merged = part[0].astype(jnp.float32) * (weights[0] / total)
        for n, w in zip(slots[1:], weights[1:]):
            merged = merged + part[n].astype(jnp.float32) * (w / total)
        ob[...] = ordered(merged.astype(jnp.bfloat16)[:, :SPAN])
        keep(ob, rs, own_b, 0).start()
        deliver(ob, rs, 0, own_b, 0)

    def attend_text():
        arrived(txt.at[1 - core], text_recv.at[2])
        land(cb_h, cb.at[pl.ds(0, SPAN)], 6, 6)()
        land(ca_h, ca, 7, 7)()
        keys_b, values_b = text_rows(1, 0), text_rows(1, 1).T
        keys, values_t = text_rows(0, 0), text_rows(0, 1).T
        peak_b = text_scores(cb[...], keys_b, s0)
        peak = text_scores(ca[a_tiles[0][0], :], keys, s1)
        result_b = text_mix(s0, WIDE, peak_b, values_b)
        for n, (cols, _) in enumerate(a_tiles):
            if n + 1 < len(a_tiles):
                ahead = text_scores(ca[a_tiles[n + 1][0], :], keys, held[n % 2])
            ot[:, cols] = text_mix(held[(n + 1) % 2], TILE, peak, values_t)
            peak = ahead
            if n > 0:
                oc[n - 1] = ordered(ot[:, (n - 1) * SPAN : n * SPAN])
                deliver(oc.at[n - 1], rc, n % NX, own_a, 1)
        keep(oc.at[NX - 1], rc, own_a, 2).start()
        od[...] = ordered(result_b[:, :SPAN])
        keep(od, rc, own_b, 1).start()
        deliver(od, rc, 0, own_b, 1)

    def region_of(i):
        theirs = jnp.logical_or(i == 1, jnp.logical_or(jnp.logical_or(i == 4, i == 5), i == 7))
        cc = jnp.where(theirs, 1 - core, core)
        yy = jnp.where(i < 2, y, jnp.where(i >= 6, yo, jnp.where(lax.rem(i, 2) == 0, ym, yp)))
        return cc, yy, cc * NY + yy

    def a_scores(region, cols, into):
        cc, yy, at = region
        q_tile = qa[cols, :]
        s = lax.dot_general(ka[at, : REGION - SPAN, :], q_tile, NT, preferred_element_type=jnp.float32)
        into[: REGION - SPAN, :TILE] = s
        e = lax.dot_general(ka[at, REGION - SPAN :, :], q_tile, NT, preferred_element_type=jnp.float32)
        e = masked(e, cc, yy, limit)
        into[REGION - SPAN :, :TILE] = e
        return jnp.maximum(jnp.max(s, axis=0, keepdims=True), jnp.max(e, axis=0, keepdims=True))

    def a_region(i, carry):
        region = region_of(i)

        @pl.when(i == 1)
        def _():
            for t in range(2):
                arrived(a[t].at[region[2]], twin_recv.at[0, t])

        @pl.when(i == 2)
        def _():
            pass_on(1)
            merge_parts()

        @pl.when(i == 3)
        def _():
            attend_text()

        vt[...] = va[region[2]].T
        attend(a_tiles, TILE, lambda cols, into: a_scores(region, cols, into))
        return carry

    land(qa_h, qa, 5, 5)()
    lax.fori_loop(0, 4, a_region, 0)
    took(a, a_half(yo, 0), 6)
    took(a, a_half(yo, 1), 7)
    share(a, a_y(yo), 3)

    last = [region_of(i) for i in (4, 5, 6, 7)]
    for (cc, yy, at), n in ((last[0], 1), (last[1], 2), (last[3], 3)):
        for t in range(2):
            arrived(a[t].at[at], twin_recv.at[n, t])
    for n, region in enumerate(last):
        vt4[n] = va[region[2]].T

    def a_tile(t, peak):
        cols = pl.ds(pl.multiple_of(t * TILE, TILE), TILE)
        after = pl.ds(pl.multiple_of(jnp.minimum(t + 1, REGION // TILE - 1) * TILE, TILE), TILE)
        for n in range(4):
            if n < 3:
                ahead = a_scores(last[n + 1], cols, held[(n + 1) % 2])
            else:
                ahead = a_scores(last[0], after, held[0])
            absorb(cols, TILE, held[n % 2], peak, vt4.at[n])
            peak = ahead
        ot[:, cols] = (acc[:, cols] / row_l[0:1, cols]).astype(jnp.bfloat16)
        for n in range(NX):
            @pl.when(t == n + 1)
            def _():
                oa[n] = ordered(ot[:, n * SPAN : (n + 1) * SPAN])
                if n == NX - 1:
                    keep(oa.at[n], rs, own_a, 3).start()
                deliver(oa.at[n], rs, (n + 1) % NX, own_a, 0)
        return peak

    lax.fori_loop(0, REGION // TILE, a_tile, a_scores(last[0], slice(0, TILE), held[0]))

    for n in range(4):
        arrived(v.at[:, pl.ds(0, (NX * NZ - 1 + NZ - 1) * HD)], send.at[n])
    for t in range(2):
        for n in (0, 1):
            arrived(b_y(y)(b[t]), ring_send.at[n, t])
            arrived(b_half(y, 0)(b[t]), ring_send.at[2 + n, t])
            arrived(a_y(y)(a[t]), ring_send.at[4 + n, t])
            arrived(a_half(y, 0)(a[t]), ring_send.at[6 + n, t])
        for n in range(4):
            arrived(a_y(y)(a[t]), twin_send.at[n, t])
        arrived(b[t].at[core], twin_send.at[4, t])
    for n in range(1, NX):
        arrived(qb.at[n, pl.ds(0, SPAN)], fan_send.at[n - 1])
        arrived(part.at[n], part_send.at[n - 1, 0])
        arrived(stat.at[n], part_send.at[n - 1, 1])
    arrived(txt.at[core, y, pl.ds(0, NX - 1)], text_send.at[0])

    @pl.when(zl != core)
    def _():
        arrived(txt.at[core, y, 0], text_send.at[3])

    arrived(txt.at[core, pl.ds(0, NY - 1)], text_send.at[1])
    arrived(txt.at[core], text_send.at[2])
    keep(ob, rs, own_b, 0).wait()
    keep(od, rc, own_b, 1).wait()
    keep(oc.at[NX - 1], rc, own_a, 2).wait()
    keep(oa.at[NX - 1], rs, own_a, 3).wait()
    for n, r, out in ((1, rc, out_c), (0, rs, out_s)):
        moved = r.at[:, :, pl.ds(0, (others + NZ * NC - 1) // 2 * HD)]
        arrived(moved, out_recv.at[n])
        out[...] = sum(jnp.dot(rows_to_own(cc), r[cc], preferred_element_type=jnp.float32)
                       for cc in range(NC)).astype(jnp.bfloat16)
        arrived(moved, out_send.at[n])


def rows_to_own(core):
    to = lax.broadcasted_iota(jnp.int32, (TOK, PIECE), 0)
    piece = lax.broadcasted_iota(jnp.int32, (TOK, PIECE), 1)
    return jnp.where(to == piece + (piece // TW) * TW + core * TW, 1.0, 0.0).astype(jnp.bfloat16)


def block(pad, q, k, v, c, text_key, text_value):
    any_spec = pl.BlockSpec(memory_space=pl.ANY)
    vmem = pl.BlockSpec(memory_space=pltpu.VMEM)
    dma = pltpu.SemaphoreType.DMA
    half = lambda *s: pltpu.VMEM(s, jnp.bfloat16)
    full = lambda *s: pltpu.VMEM(s, jnp.float32)
    landing = [REGION, REGION, SPAN, SPAN, REGION, REGION, SPAN, SPAN]
    result = jax.ShapeDtypeStruct((TOK, HEADS * HD), jnp.bfloat16)
    return pl.pallas_call(
        block_kernel,
        in_specs=[any_spec] * 8,
        out_specs=[vmem] * 2 + [any_spec] * 8,
        out_shape=[result] * 2 + [jax.ShapeDtypeStruct((n, HD), jnp.bfloat16) for n in landing],
        scratch_shapes=[
            pltpu.SMEM((1,), jnp.int32), full(8, HD), half(GROUPS * PAD, SPAN), pltpu.VMEM((SPAN, HD), jnp.int32),
            half(NC, PIECE, HEADS * HD), half(NC, PIECE, HEADS * HD),
            half(TOK, HEADS * HD), half(TOK, HEADS * HD), half(HEADS, TOK, HD), half(HEADS, TOK, HD),
            half(REGION, HD), half(NX, WIDE, HD), half(REGION, HD), half(WIDE, HD),
            half(NC * NY, REGION, HD), half(NC * NY, REGION, HD), half(NC, NY, SPAN, HD), half(NC, NY, SPAN, HD),
            half(NC, NY, NX, 2, 2, 16, HD),
            full(REGION, WIDE), full(REGION, WIDE), half(HD, REGION), half(4, HD, REGION), full(HD, NX * WIDE),
            full(8, NX * WIDE), full(8, NX * WIDE), half(HD, REGION),
            half(NX, GROUPS, PIECE, HD), half(GROUPS, PIECE, HD), half(NX, GROUPS, PIECE, HD), half(GROUPS, PIECE, HD),
            half(2 * NX, HD, WIDE), full(2 * NX, 8, WIDE),
            dma((4,)), dma((8,)), dma((12,)), dma((8, 2)), dma((8, 2)), dma((5, 2)), dma((5, 2)), dma((3,)), dma((3,)),
            dma((3, 2)), dma((3, 2)), dma((4,)), dma((3,)), dma((2,)), dma((2,)), dma((4,)),
        ],
        compiler_params=pltpu.CompilerParams(collective_id=0, has_side_effects=True),
        name="block",
    )(pad, omega_table(), q, k, v, c, text_key, text_value)[:2]


def omega_table():
    pair = np.arange(HD) // 2
    side = HD // 6
    first = HD // 2 - 2 * side
    table = np.zeros((8, HD), np.float32)
    for axis, start, count in ((0, 0, first), (1, first, side), (2, first + side, side)):
        inside = (pair >= start) & (pair < start + count)
        table[axis] = np.where(inside, 10000.0 ** (-((pair - start) / count)), 0.0)
    table[3] = np.where(np.arange(HD) % 2 == 0, -1.0, 1.0)
    return jnp.asarray(table)


def body(self_query, self_key, self_value, cross_query, text_key, text_value, padded_count):
    return tuple(block(padded_count, self_query, self_key, self_value, cross_query, text_key, text_value))


def solution(mesh):
    split = Mesh(mesh.devices.reshape(4, 4, 2, 4, 2), BLK + ULY)
    own = P(BLK + ULY, None)
    return jax.shard_map(body, mesh=split, in_specs=(own,) * 4 + (P(BLK, ULY),) * 2 + (P(),),
                         out_specs=(own, own), check_vma=False)
```
